32 devices in a mesh: fy: 2 (over x), fx: 8 (over z, y), ch: 2 (over core).
Axes of the slice: x: 2, y: 2, z: 4, core: 2. Of those that a mesh axis runs over, the one named last changes fastest.
Arguments:
- image_cube: float32 [64, 512, 416], P('ch', 'fx', 'fy'), may hold values from 0 to 2
- data_grad: bfloat16 [64, 512, 416], P('ch', 'fx', 'fy'), may hold values from -6 to 6
- dual_coeffs: float32 [64, 896, 512], P('ch', 'fx', 'fy'), may hold values from -6 to 6
- reweights: float32 [896, 512], P('fx', 'fy'), may hold values from 1 to 40
Outputs:
- image_next: float32 [64, 512, 416], P('ch', 'fx', 'fy')
- dual_next: float32 [64, 896, 512], P('ch', 'fx', 'fy')
The draws below stay inside these ranges and needn't reach their ends.
All inputs are finite; a program needn't handle non-finite values.
Results may differ from the reference program's by a relative error of at most 0.0003.
Values sent between devices are 32-bit elements; how exact they have to be, the bound alone decides.
A program may use at most 64 MiB of HBM per device.

```python
import math
import jax
import jax.numpy as jnp
import numpy as np
from jax import lax

CH = 64
LEVELS = 2
TX = 64
TY = 208
INTERSECTION = 48
EX = 112
EY = 256
NX = 512
NY = 416
N_FY = 2
N_FX = 8


def steps_of(own_key, dims, shards, low, top_value):
    def one(position, blocks):
        steps = jax.random.uniform(jax.random.fold_in(jax.random.fold_in(own_key, 6), position), (blocks,), jnp.float32, low / len(shards), top_value / len(shards))
        return jnp.repeat(jnp.exp(steps), dims[position] // blocks).reshape((-1,) + (1,) * (len(dims) - position - 1))

    factor_of = one(*shards[0])
    for cut in shards[1:]:
        factor_of = factor_of * one(*cut)
    return factor_of


def noise(stream_key, dims, width, limit, pieces=(), kind=jnp.bfloat16):
    loudness = steps_of(stream_key, dims, pieces, -0.22, 0.18) if pieces else 1.0
    array = jax.random.normal(stream_key, dims, jnp.float32) * width * loudness
    return jnp.minimum(jnp.maximum(array, -limit), limit).astype(kind)


def setup_inputs(seed: int = 0) -> dict:
    keys = jax.random.split(jax.random.key(seed), 5)
    return {
        "image_cube": jnp.clip(2.0 * jax.random.uniform(keys[0], (CH, NX, NY), jnp.float32) ** steps_of(keys[0], (CH, NX, NY), ((0, 2), (1, 8), (2, 2)), -0.2, 0.2), 0.0, 2.0),
        "data_grad": noise(keys[1], (CH, NX, NY), 1.0, 6.0, ((0, 2), (1, 8), (2, 2))),
        "dual_coeffs": noise(keys[2], (CH, N_FX * EX, N_FY * EY), 1.0, 6.0, ((0, 2), (1, 8), (2, 2)), jnp.float32),
        "reweights": jnp.clip(jnp.exp(math.log(40.0) - 3.6888795 * jax.random.uniform(keys[3], (N_FX * EX, N_FY * EY), jnp.float32) ** steps_of(keys[3], (N_FX * EX, N_FY * EY), ((0, 8), (1, 2)), -0.2, 0.2)), 1.0, 40.0),
    }


LOW_PASS = [-0.00011747678400228192, 0.0006754494059985568, -0.0003917403729959771, -0.00487035299301066, 0.008746094047015655, 0.013981027917015516, -0.04408825393106472, -0.01736930100202211, 0.128747426620186, 0.00047248457399797254, -0.2840155429624281, -0.015829105256023893, 0.5853546836548691, 0.6756307362980128, 0.3128715909144659, 0.05441584224308161]
TAU_STEP = 0.5
LAMBDA_REG = 1.0
EPSILON = 1e-06

def level_matrix(length):
    halved = length // 2
    taps_count = len(LOW_PASS)
    matrix = np.zeros((length, length))
    for out_row in range(halved):
        for tap_index in range(taps_count):
            column = (2 * out_row + tap_index) % length
            matrix[out_row, column] += LOW_PASS[tap_index]
            matrix[halved + out_row, column] += (-1) ** tap_index * LOW_PASS[taps_count - 1 - tap_index]
    return matrix

def analysis(facet_block, levels):
    result = facet_block
    width_x = facet_block.shape[1]
    width_y = facet_block.shape[2]
    for level_step in range(levels):
        matrix_x = jnp.asarray(level_matrix(width_x), dtype=facet_block.dtype)
        matrix_y = jnp.asarray(level_matrix(width_y), dtype=facet_block.dtype)
        corner_part = result[:, :width_x, :width_y]
        corner_part = jnp.einsum('cxy,vy->cxv', corner_part, matrix_y, precision=lax.Precision.HIGHEST)
        corner_part = jnp.einsum('ux,cxv->cuv', matrix_x, corner_part, precision=lax.Precision.HIGHEST)
        result = result.at[:, :width_x, :width_y].set(corner_part)
        width_x = width_x // 2
        width_y = width_y // 2
    return result

def synthesis(coeff_block, levels):
    result = coeff_block
    for level_step in range(levels - 1, -1, -1):
        width_x = coeff_block.shape[1] // 2 ** level_step
        width_y = coeff_block.shape[2] // 2 ** level_step
        matrix_x = jnp.asarray(level_matrix(width_x), dtype=coeff_block.dtype)
        matrix_y = jnp.asarray(level_matrix(width_y), dtype=coeff_block.dtype)
        corner_part = result[:, :width_x, :width_y]
        corner_part = jnp.einsum('ux,cuv->cxv', matrix_x, corner_part, precision=lax.Precision.HIGHEST)
        corner_part = jnp.einsum('cxv,vy->cxy', corner_part, matrix_y, precision=lax.Precision.HIGHEST)
        result = result.at[:, :width_x, :width_y].set(corner_part)
    return result

def cover_weights(total, tile, intersection, count, float_kind):
    positions = jnp.arange(total, dtype=jnp.int32)
    offsets = positions % tile
    owners = positions // tile
    edge = (offsets >= tile - intersection) & (owners < count - 1)
    return jnp.where(edge, 0.5 ** 0.5, 1.0).astype(float_kind)

def reference(image_cube, data_grad, dual_coeffs, reweights):
    float_kind = image_cube.dtype
    weight_map = cover_weights(NX, TX, INTERSECTION, N_FX, float_kind)[:, None] * cover_weights(NY, TY, INTERSECTION, N_FY, float_kind)[None, :]
    facets = N_FX * N_FY
    anchor = jnp.int32(0)

    def add_facet(facet_number, accumulated):
        col_index = (facet_number // N_FY).astype(jnp.int32)
        row_index = (facet_number % N_FY).astype(jnp.int32)
        coeff_block = lax.dynamic_slice(dual_coeffs, (anchor, col_index * EX, row_index * EY), (CH, EX, EY))
        piece = synthesis(coeff_block, LEVELS)
        start = (anchor, col_index * TX, row_index * TY)
        current = lax.dynamic_slice(accumulated, start, (CH, EX, EY))
        return lax.dynamic_update_slice(accumulated, current + piece, start)
    accumulated = jnp.zeros((CH, NX + INTERSECTION, NY + INTERSECTION), float_kind)
    accumulated = lax.fori_loop(0, facets, add_facet, accumulated)
    adjoint = accumulated[:, INTERSECTION:, INTERSECTION:] * weight_map
    image_next = jnp.maximum(image_cube - TAU_STEP * (data_grad.astype(float_kind) + adjoint), 0.0)
    extrap = (2.0 * image_next - image_cube) * weight_map
    padded = jnp.pad(extrap, ((0, 0), (INTERSECTION, 0), (INTERSECTION, 0)))

    def new_facet(facet_number, result):
        col_index = (facet_number // N_FY).astype(jnp.int32)
        row_index = (facet_number % N_FY).astype(jnp.int32)
        window = lax.dynamic_slice(padded, (anchor, col_index * TX, row_index * TY), (CH, EX, EY))
        place = (anchor, col_index * EX, row_index * EY)
        updated = lax.dynamic_slice(dual_coeffs, place, (CH, EX, EY)) + analysis(window, LEVELS)
        squared_sum = lax.optimization_barrier(jnp.sum(updated * updated, axis=0))
        local_weights = lax.dynamic_slice(reweights, (col_index * EX, row_index * EY), (EX, EY))
        factor = jnp.minimum(1.0, LAMBDA_REG * local_weights / jnp.sqrt(squared_sum + EPSILON))
        return lax.dynamic_update_slice(result, updated * factor[None], place)
    dual_next = lax.fori_loop(0, facets, new_facet, jnp.zeros_like(dual_coeffs))
    return (image_next, dual_next)
```

```python
import functools

import jax
import jax.numpy as jnp
import numpy as np
from jax import lax
from jax.experimental import pallas as pl
from jax.experimental.pallas import tpu as pltpu
from jax.sharding import PartitionSpec as P

LEVELS = 2
LOW_PASS = [
    -0.00011747678400228192,
    0.0006754494059985568,
    -0.0003917403729959771,
    -0.00487035299301066,
    0.008746094047015655,
    0.013981027917015516,
    -0.04408825393106472,
    -0.01736930100202211,
    0.128747426620186,
    0.00047248457399797254,
    -0.2840155429624281,
    -0.015829105256023893,
    0.5853546836548691,
    0.6756307362980128,
    0.3128715909144659,
    0.05441584224308161,
]
TAU_STEP = 0.5
LAMBDA_REG = 1.0
EPSILON = 1e-06
LANES = 128
CHUNK = 2
AT_B, AT_VIA_L, AT_C, AT_VIA_R, AT_D, AT_E = 1, 2, 3, 5, 6, 8
MESH = pl.DeviceIdType.MESH
F32 = jnp.float32
BF16 = jnp.bfloat16


def level_matrix(length):
    halved = length // 2
    taps_count = len(LOW_PASS)
    matrix = np.zeros((length, length))
    for out_row in range(halved):
        for tap_index in range(taps_count):
            column = (2 * out_row + tap_index) % length
            matrix[out_row, column] += LOW_PASS[tap_index]
            matrix[halved + out_row, column] += (-1) ** tap_index * LOW_PASS[
                taps_count - 1 - tap_index
            ]
    return matrix


def halves(matrix):
    exact = np.asarray(matrix, np.float32)
    high = exact.astype(BF16)
    low = (exact - high.astype(np.float32)).astype(BF16)
    return high, low


def right_factor(matrix):
    high, low = halves(matrix)
    return jnp.asarray(np.concatenate([high, low, high], axis=0))


def left_factor(matrix, padded):
    high, low = halves(np.pad(matrix, ((0, 0), (0, padded - matrix.shape[1]))))
    return jnp.asarray(np.concatenate([high, low, high], axis=1))


def round_up(value, to):
    return -(-value // to) * to


def split(x):
    high = x.astype(BF16)
    low = (x - high.astype(F32)).astype(BF16)
    return high, low


def times_right(x, factor):
    n, rows, columns = x.shape
    high, low = split(x.reshape(n * rows, columns))
    out = jnp.dot(jnp.concatenate([high, high, low], axis=1), factor, preferred_element_type=F32)
    return out.reshape(n, rows, out.shape[1])


def times_left(factor, x):
    rows = x.shape[0]
    padded = round_up(rows, 16)
    if padded > rows:
        x = jnp.concatenate([x, jnp.zeros((padded - rows, x.shape[1]), F32)], axis=0)
    high, low = split(x)
    return jnp.dot(factor, jnp.concatenate([high, high, low], axis=0), preferred_element_type=F32)


def corner_step(corner, right, left):
    n = corner.shape[0]
    width = corner.shape[2]
    mid = times_right(corner, right)
    pieces = []
    for c in range(0, n, 2):
        pair = times_left(left, jnp.concatenate([mid[c], mid[c + 1]], axis=1))
        pieces += [pair[:, :width], pair[:, width:]]
    return pieces


def kernel(
    names,
    image_hbm, grad_hbm, dual_hbm, rew_hbm,
    sy0_hbm, sx0_hbm, sy1_hbm, sx1_hbm, ay0_hbm, ax0_hbm, ay1_hbm, ax1_hbm,
    next_ref, upd_ref, factor_ref,
    sy0_ref, sx0_ref, sy1_ref, sx1_ref, ay0_ref, ax0_ref, ay1_ref, ax1_ref, rew_ref,
    image, grad, dual, work, y1s, y1r, ls, lr, rs, rr, y2s, y2r, via, acc, accr,
    in_sem, const_sem, send_sem, recv_sem, via_send, via_recv, ch_send, ch_recv,
):
    fy_name, fx_name, ch_name = names
    channels, tx, ty = image.shape
    ex, ey = dual.shape[1:]
    border = ex - tx
    n = CHUNK
    chunks = channels // n
    half = ex // 2
    tail = ty - LANES
    packed = ls.shape[1]
    fy, fx, ch = (lax.axis_index(a) for a in names)
    n_fy, n_fx, n_ch = (lax.axis_size(a) for a in names)
    has_up, has_down = fy > 0, fy < n_fy - 1
    has_left, has_right = fx > 0, fx < n_fx - 1

    barrier = pltpu.get_barrier_semaphore()
    near = (
        (has_up, {fy_name: fy - 1}),
        (has_down, {fy_name: fy + 1}),
        (has_left, {fx_name: fx - 1}),
        (has_right, {fx_name: fx + 1}),
        (fx > 1, {fx_name: fx - 2}),
        (fx < n_fx - 2, {fx_name: fx + 2}),
    )
    for there, where in near:
        @pl.when(there)
        def _(where=where):
            pl.semaphore_signal(barrier, inc=1, device_id=where, device_id_type=MESH)
    for step in range(1, n_ch):
        pl.semaphore_signal(
            barrier, inc=1, device_id={ch_name: lax.rem(ch + step, n_ch)}, device_id_type=MESH
        )

    def part(k):
        return pl.ds(k * n, n)

    def load(k, which):
        src, dst = ((dual_hbm, dual), (image_hbm, image), (grad_hbm, grad))[which]
        return pltpu.make_async_copy(src.at[part(k)], dst.at[part(k)], in_sem.at[which, k])

    constants = (
        (sy1_hbm, sy1_ref), (sx1_hbm, sx1_ref), (sy0_hbm, sy0_ref), (sx0_hbm, sx0_ref),
        (ay0_hbm, ay0_ref), (ax0_hbm, ax0_ref), (ay1_hbm, ay1_ref), (ax1_hbm, ax1_ref),
        (rew_hbm, rew_ref),
    )

    def constant(i):
        src, dst = constants[i]
        return pltpu.make_async_copy(src, dst, const_sem.at[i])

    whole, first_rows, last_rows = pl.ds(0, packed), pl.ds(0, border), pl.ds(border, packed - border)
    corner_half, own_half = border // 2, tx // 2
    corner_rows, own_rows = pl.ds(0, corner_half), pl.ds(corner_half, own_half)
    links = (
        (y1s, y1r, {fy_name: fy - 1}, pl.ds(0, half), 0),
        (ls, lr, {fx_name: fx - 1}, first_rows, 1),
        (ls, lr, {fx_name: fx - 1}, last_rows, 1),
        (rs, rr, {fx_name: fx + 1}, whole, 2),
        (y2s, y2r, {fy_name: fy + 1}, own_rows, 3),
        (y2s, y2r, {fy_name: fy + 1}, corner_rows, 3),
    )
    UP, LEFT_A, LEFT_B, RIGHT, DOWN_A, DOWN_B = range(6)

    def link(c, which):
        src, dst, where, rows, sent = links[which]
        return pltpu.make_async_remote_copy(
            src_ref=src.at[c, rows],
            dst_ref=dst.at[c, rows],
            send_sem=send_sem.at[sent],
            recv_sem=recv_sem.at[which, c],
            device_id=where,
            device_id_type=MESH,
        )

    def sent_all(which):
        src, dst, where, _, sent = links[which]
        return pltpu.make_async_remote_copy(
            src_ref=src,
            dst_ref=dst,
            send_sem=send_sem.at[sent],
            recv_sem=recv_sem.at[which, 0],
            device_id=where,
            device_id_type=MESH,
        )

    odd = lax.rem(fx, 2) == 1
    groups = n_fx // 2

    def turn(c, m):
        return ((c + 1) * m) // groups - (c * m) // groups == 1

    def leftward(which):
        return which != RIGHT

    def sends_via(c, which):
        if leftward(which):
            return jnp.logical_not(odd) & has_left & has_right & turn(c, fx // 2)
        return odd & has_left & has_right & jnp.logical_not(turn(c, (fx + 1) // 2))

    def to_via(c, which):
        src, _, _, rows, sent = links[which]
        return pltpu.make_async_remote_copy(
            src_ref=src.at[c, rows],
            dst_ref=via.at[c, rows],
            send_sem=send_sem.at[sent],
            recv_sem=via_recv.at[which, c],
            device_id={fx_name: fx + 1 if leftward(which) else fx - 1},
            device_id_type=MESH,
        )

    def passes_on(c, which):
        if leftward(which):
            return odd & (fx > 2) & turn(c, fx // 2)
        return jnp.logical_not(odd) & (fx < n_fx - 2) & jnp.logical_not(turn(c, (fx + 2) // 2))

    def from_via(c, which):
        _, dst, _, rows, _ = links[which]
        return pltpu.make_async_remote_copy(
            src_ref=via.at[c, rows],
            dst_ref=dst.at[c, rows],
            send_sem=via_send.at[which, c],
            recv_sem=recv_sem.at[which, c],
            device_id={fx_name: fx - 2 if leftward(which) else fx + 2},
            device_id_type=MESH,
        )

    def stage_via(ways, k):
        for j in range(n):
            c = k * n + j

            @pl.when(passes_on(c, ways[0]))
            def _(c=c):
                for way in ways:
                    to_via(c, way).wait_recv()
                    from_via(c, way).start()

    def to_side(c, which):
        around = sends_via(c, which)

        @pl.when(around)
        def _():
            to_via(c, which).start()

        @pl.when(jnp.logical_not(around))
        def _():
            link(c, which).start()

    load(0, 0).start()
    for i in range(4):
        constant(i).start()

    def loads(k, carry):
        load(k, 0).start()
        return carry

    def more_loads(k, carry):
        load(k, 1).start()
        load(k, 2).start()
        return carry

    lax.fori_loop(1, chunks, loads, 0)
    lax.fori_loop(0, chunks, more_loads, 0)
    for i in range(4, 9):
        constant(i).start()
    acc[...] = jnp.zeros_like(acc)

    peers = n_ch - 1
    for at, size in ((fy, n_fy), (fx, n_fx)):
        peers = peers + jnp.minimum(at, 1) + jnp.minimum(size - 1 - at, 1)
    peers = peers + jnp.minimum(fx // 2, 1) + jnp.minimum((n_fx - 1 - fx) // 2, 1)

    def lanes(rows):
        return lax.broadcasted_iota(jnp.int32, (rows, LANES), 1)

    def own_edge(rows):
        at = lanes(rows)
        return (at >= tail - border) & (at < tail)

    def roll(x, by):
        return pltpu.roll(x, by % LANES, 1)

    g = border // 3

    def pack_rest(rest, buffer, c):
        a, b, d = rest[:g], rest[g:2 * g], rest[2 * g:]
        low = lanes(g) < tail
        buffer[c, border:border + g] = jnp.where(low, a, roll(b, tail))
        buffer[c, border + g:] = jnp.where(low, d, roll(b, 2 * tail - LANES))

    def unpacked(buffer, c):
        p, q = buffer[c, border:border + g], buffer[c, border + g:]
        b = jnp.where(lanes(g) < LANES - tail, roll(p, -tail), roll(q, LANES - 2 * tail))
        return buffer[c, :border], jnp.concatenate([p, b, q], axis=0)

    half_lane = LANES // 2

    def stage_a(k):
        load(k, 0).wait()

        @pl.when(k == 0)
        def _():
            for i in range(4):
                constant(i).wait()

        x = dual[part(k)]
        hx, hy = ex // 2, ey // 2
        corner = corner_step(x[:, :hx, :hy], sy1_ref[...], sx1_ref[...])
        full = jnp.stack(
            [
                jnp.concatenate(
                    [jnp.concatenate([corner[j], x[j, :hx, hy:]], axis=1), x[j, hx:]], axis=0
                )
                for j in range(n)
            ]
        )
        mid = times_right(full, sy0_ref[...])
        for j in range(n):
            work[k * n + j] = times_left(sx0_ref[...], mid[j])

        @pl.when(k == 0)
        def _():
            pl.semaphore_wait(barrier, peers)

        @pl.when(has_up)
        def _():
            edge = own_edge(half)
            for j in range(n):
                c = k * n + j
                first, second = work[c, :half, LANES:], work[c, half:, LANES:]
                y1s[c] = jnp.where(edge, roll(first, -border), roll(second, half_lane - border))
                link(c, UP).start()

        @pl.when(has_left)
        def _():
            for j in range(n):
                c = k * n + j
                ls[c, :border] = work[c, :border, :LANES]
                to_side(c, LEFT_A)

    def stage_b(k):
        for j in range(n):
            c = k * n + j

            @pl.when(has_down)
            def _(c=c):
                link(c, UP).wait_recv()
                edge = own_edge(half)
                got = y1r[c]
                work[c, :half, LANES:] += jnp.where(edge, got, 0.0)
                work[c, half:, LANES:] += jnp.where(edge, roll(got, half_lane), 0.0)

            @pl.when(has_left)
            def _(c=c):
                pack_rest(work[c, :border, LANES:], ls, c)
                to_side(c, LEFT_B)

    def stage_c(k):
        load(k, 1).wait()
        load(k, 2).wait()
        xs = lax.broadcasted_iota(jnp.int32, (tx, ty), 0)
        ys = lax.broadcasted_iota(jnp.int32, (tx, ty), 1)
        ax = jnp.where((xs >= tx - border) & has_right, 0.5**0.5, 1.0).astype(F32)
        by = jnp.where((ys >= ty - border) & has_down, 0.5**0.5, 1.0).astype(F32)
        weight = ax * by
        for j in range(n):
            c = k * n + j

            @pl.when(has_right)
            def _(c=c):
                link(c, LEFT_A).wait_recv()
                link(c, LEFT_B).wait_recv()
                main, rest = unpacked(lr, c)
                work[c, ex - border:, :LANES] += main
                work[c, ex - border:, LANES:] += rest

            adjoint = work[c, border:, :ty] * weight
            current = image[c]
            fresh = jnp.maximum(current - TAU_STEP * (grad[c].astype(F32) + adjoint), 0.0)
            work[c, border:, :ty] = (2.0 * fresh - current) * weight
            next_ref[c] = fresh

            @pl.when(has_right)
            def _(c=c):
                rs[c, :border] = work[c, ex - border:, :LANES]
                pack_rest(work[c, ex - border:, LANES:], rs, c)
                to_side(c, RIGHT)

            @pl.when(has_down)
            def _(c=c):
                mid = border + own_half
                y2s[c, corner_half:] = jnp.where(
                    own_edge(own_half), work[c, border:mid, LANES:], roll(work[c, mid:, LANES:], half_lane)
                )
                link(c, DOWN_A).start()

    def stage_d(k):
        for j in range(n):
            c = k * n + j

            @pl.when(has_left)
            def _(c=c):
                link(c, RIGHT).wait_recv()
                main, rest = unpacked(rr, c)
                work[c, :border, :LANES] = main
                work[c, :border, LANES:] = rest

            @pl.when(jnp.logical_not(has_left))
            def _(c=c):
                work[c, :border] = jnp.zeros((border, ey), F32)

            @pl.when(has_down)
            def _(c=c):
                y2s[c, :corner_half] = jnp.where(
                    own_edge(corner_half),
                    work[c, :corner_half, LANES:],
                    roll(work[c, corner_half:border, LANES:], half_lane),
                )
                link(c, DOWN_B).start()

    def stage_e(k):
        @pl.when(k == 0)
        def _():
            for i in range(4, 8):
                constant(i).wait()

        for j in range(n):
            c = k * n + j
            for way in (LEFT_A, LEFT_B, RIGHT):
                @pl.when(passes_on(c, way))
                def _(c=c, way=way):
                    from_via(c, way).wait_send()

        @pl.when(has_up)
        def _():
            for j in range(n):
                c = k * n + j
                link(c, DOWN_A).wait_recv()
                link(c, DOWN_B).wait_recv()
                for at, rows, buffered in ((0, corner_half, 0), (border, own_half, corner_half)):
                    low = lanes(rows) < tail
                    got = y2r[c, buffered:buffered + rows]
                    first, second = pl.ds(at, rows), pl.ds(at + rows, rows)
                    work[c, first, LANES:] = jnp.where(low, work[c, first, LANES:], roll(got, border))
                    work[c, second, LANES:] = jnp.where(
                        low, work[c, second, LANES:], roll(got, border - half_lane)
                    )

        @pl.when(jnp.logical_not(has_up))
        def _():
            low = lanes(ex) < tail
            for j in range(n):
                c = k * n + j
                work[c, :, LANES:] = jnp.where(low, work[c, :, LANES:], 0.0)

        mid = times_right(work[part(k)], ay0_ref[...])
        hx, hy = ex // 2, ey // 2
        full = [times_left(ax0_ref[...], mid[j]) for j in range(n)]
        corner = corner_step(jnp.stack([f[:hx, :hy] for f in full]), ay1_ref[...], ax1_ref[...])
        total = acc[...]
        for j in range(n):
            c = k * n + j
            coeffs = jnp.concatenate(
                [jnp.concatenate([corner[j], full[j][:hx, hy:]], axis=1), full[j][hx:]], axis=0
            )
            updated = dual[c] + coeffs
            total = total + updated * updated
            upd_ref[c] = updated
        acc[...] = total

    stages = (
        (0, stage_a),
        (AT_B, stage_b),
        (AT_VIA_L, functools.partial(stage_via, (LEFT_A, LEFT_B))),
        (AT_VIA_R, functools.partial(stage_via, (RIGHT,))),
        (AT_C, stage_c),
        (AT_D, stage_d),
        (AT_E, stage_e),
    )

    def step(t, carry):
        for delay, stage in stages:
            @pl.when((t >= delay) & (t < chunks + delay))
            def _(delay=delay, stage=stage):
                stage(t - delay)
        return carry

    lax.fori_loop(0, chunks + AT_E, step, 0)

    def across(step):
        return pltpu.make_async_remote_copy(
            src_ref=acc,
            dst_ref=accr.at[step - 1],
            send_sem=ch_send.at[step - 1],
            recv_sem=ch_recv.at[step - 1],
            device_id={ch_name: lax.rem(ch + step, n_ch)},
            device_id_type=MESH,
        )

    for s in range(1, n_ch):
        across(s).start()
    for which, there in ((UP, has_up), (LEFT_A, has_left), (RIGHT, has_right), (DOWN_A, has_down)):
        @pl.when(there)
        def _(which=which):
            sent_all(which).wait_send()
    constant(8).wait()
    for s in range(1, n_ch):
        across(s).wait()
    total = acc[...]
    for s in range(1, n_ch):
        total = total + accr[s - 1]
    factor_ref[...] = jnp.minimum(1.0, LAMBDA_REG * rew_ref[...] / jnp.sqrt(total + EPSILON))


def shards(names, image_cube, data_grad, dual_coeffs, reweights):
    channels, tx, ty = image_cube.shape
    _, ex, ey = dual_coeffs.shape
    border = ex - tx
    n_ch = lax.axis_size(names[2])
    chunks = channels // CHUNK
    packed = border + 2 * (border // 3)
    wy0 = np.roll(level_matrix(ey), -(ey - ty), axis=1)
    wx0 = level_matrix(ex)
    wy1, wx1 = level_matrix(ey // 2), level_matrix(ex // 2)
    px0, px1 = round_up(ex, 16), round_up(ex // 2, 16)
    factors = (
        right_factor(wy0), left_factor(wx0.T, px0), right_factor(wy1), left_factor(wx1.T, px1),
        right_factor(wy0.T), left_factor(wx0, px0), right_factor(wy1.T), left_factor(wx1, px1),
    )
    far = pl.BlockSpec(memory_space=pltpu.HBM)
    inside = pl.BlockSpec(memory_space=pltpu.VMEM)
    lines = pltpu.VMEM((channels, ex // 2, LANES), F32)
    sides = pltpu.VMEM((channels, packed, LANES), F32)
    operands = (image_cube, data_grad, dual_coeffs, reweights, *factors)
    image_next, updated, factor = pl.pallas_call(
        functools.partial(kernel, names),
        out_shape=(
            pltpu.VMEM((channels, tx, ty), F32),
            pltpu.VMEM((channels, ex, ey), F32),
            pltpu.VMEM((ex, ey), F32),
        ),
        in_specs=[far] * len(operands),
        out_specs=(inside,) * 3,
        scratch_shapes=[
            *(pltpu.VMEM(f.shape, f.dtype) for f in factors),
            pltpu.VMEM((ex, ey), F32),
            pltpu.VMEM((channels, tx, ty), F32),
            pltpu.VMEM((channels, tx, ty), BF16),
            pltpu.VMEM((channels, ex, ey), F32),
            pltpu.VMEM((channels, ex, ey), F32),
            lines, lines, sides, sides, sides, sides, lines, lines, sides,
            pltpu.VMEM((ex, ey), F32),
            pltpu.VMEM((n_ch - 1, ex, ey), F32),
            pltpu.SemaphoreType.DMA((3, chunks)),
            pltpu.SemaphoreType.DMA((9,)),
            pltpu.SemaphoreType.DMA((4,)),
            pltpu.SemaphoreType.DMA((6, channels)),
            pltpu.SemaphoreType.DMA((4, channels)),
            pltpu.SemaphoreType.DMA((4, channels)),
            pltpu.SemaphoreType.DMA((n_ch - 1,)),
            pltpu.SemaphoreType.DMA((n_ch - 1,)),
        ],
        compiler_params=pltpu.CompilerParams(
            collective_id=0, has_side_effects=True, vmem_limit_bytes=40 * 2**20
        ),
        name="facets",
    )(*(pltpu.with_memory_space_constraint(a, pltpu.HBM) for a in operands))
    return image_next, updated * factor[None]


def solution(mesh):
    names = ("fy", "fx", "ch")
    return jax.shard_map(
        functools.partial(shards, names),
        mesh=mesh,
        in_specs=(P("ch", "fx", "fy"), P("ch", "fx", "fy"), P("ch", "fx", "fy"), P("fx", "fy")),
        out_specs=(P("ch", "fx", "fy"), P("ch", "fx", "fy")),
        check_vma=False,
    )
```

```python
import functools

import jax
import jax.numpy as jnp
import numpy as np
from jax import lax
from jax.experimental import pallas as pl
from jax.experimental.pallas import tpu as pltpu
from jax.sharding import PartitionSpec as P

LEVELS = 2
LOW_PASS = [
    -0.00011747678400228192,
    0.0006754494059985568,
    -0.0003917403729959771,
    -0.00487035299301066,
    0.008746094047015655,
    0.013981027917015516,
    -0.04408825393106472,
    -0.01736930100202211,
    0.128747426620186,
    0.00047248457399797254,
    -0.2840155429624281,
    -0.015829105256023893,
    0.5853546836548691,
    0.6756307362980128,
    0.3128715909144659,
    0.05441584224308161,
]
TAU_STEP = 0.5
LAMBDA_REG = 1.0
EPSILON = 1e-06
LANES = 128
SUBLANES = 8
CHUNK = 4
AT_B, AT_VIA_L, AT_C, AT_VIA_R, AT_D, AT_E = 1, 2, 3, 4, 5, 6
MESH = pl.DeviceIdType.MESH
F32 = jnp.float32
BF16 = jnp.bfloat16


def level_matrix(length):
    halved = length // 2
    taps_count = len(LOW_PASS)
    matrix = np.zeros((length, length))
    for out_row in range(halved):
        for tap_index in range(taps_count):
            column = (2 * out_row + tap_index) % length
            matrix[out_row, column] += LOW_PASS[tap_index]
            matrix[halved + out_row, column] += (-1) ** tap_index * LOW_PASS[
                taps_count - 1 - tap_index
            ]
    return matrix


def halves(matrix):
    exact = np.asarray(matrix, np.float32)
    high = exact.astype(BF16)
    low = (exact - high.astype(np.float32)).astype(BF16)
    return high, low


def right_factor(matrix):
    high, low = halves(matrix)
    return jnp.asarray(np.concatenate([high, low, high], axis=0))


def left_factor(matrix, padded):
    high, low = halves(np.pad(matrix, ((0, 0), (0, padded - matrix.shape[1]))))
    return jnp.asarray(np.concatenate([high, low, high], axis=1))


def round_up(value, to):
    return -(-value // to) * to


def split(x):
    high = x.astype(BF16)
    low = (x - high.astype(F32)).astype(BF16)
    return high, low


def times_right(x, factor):
    n, rows, columns = x.shape
    high, low = split(x.reshape(n * rows, columns))
    out = jnp.dot(jnp.concatenate([high, high, low], axis=1), factor, preferred_element_type=F32)
    return out.reshape(n, rows, out.shape[1])


def times_left(factor, x):
    rows = x.shape[0]
    padded = round_up(rows, 16)
    if padded > rows:
        x = jnp.concatenate([x, jnp.zeros((padded - rows, x.shape[1]), F32)], axis=0)
    high, low = split(x)
    return jnp.dot(factor, jnp.concatenate([high, high, low], axis=0), preferred_element_type=F32)


def corner_step(corner, right, left):
    n = corner.shape[0]
    width = corner.shape[2]
    mid = times_right(corner, right)
    pieces = []
    for c in range(0, n, 2):
        pair = times_left(left, jnp.concatenate([mid[c], mid[c + 1]], axis=1))
        pieces += [pair[:, :width], pair[:, width:]]
    return pieces


def lanes_of(rows):
    return lax.broadcasted_iota(jnp.int32, (rows, LANES), 1)


def roll(x, by):
    return pltpu.roll(x, by % LANES, 1)


def seats(border, tail):
    groups = border // SUBLANES
    bins = -(-groups * tail // LANES)
    last = groups * tail - (bins - 1) * LANES
    pieces, seat, at = [], 0, tail
    for group in range(bins, groups):
        lane = 0
        while lane < tail:
            room = LANES if seat < bins - 1 else last
            if at == room:
                seat, at = seat + 1, tail
                continue
            width = min(tail - lane, room - at)
            pieces.append((group, lane, seat, at))
            lane, at = lane + width, at + width
    spare = LANES - last
    kept = SUBLANES * last // LANES
    folds = []
    if spare:
        assert last % spare == 0 and (SUBLANES - kept) * last == spare * kept
        folds = [(row, (row - kept) * (last // spare)) for row in range(kept, SUBLANES)]
    return groups, bins, last, kept, pieces, folds


def packed_rows(border, tail):
    _, bins, _, kept, _, _ = seats(border, tail)
    return (bins - 1) * SUBLANES + kept


def pack_rest(rest, tail, buffer, c, start):
    groups, bins, last, kept, pieces, folds = seats(rest.shape[0], tail)
    lane = lanes_of(SUBLANES)
    row = lax.broadcasted_iota(jnp.int32, (SUBLANES, LANES), 0)
    part = [rest[SUBLANES * i:SUBLANES * (i + 1)] for i in range(groups)]
    out = part[:bins]
    for group, source, seat, to in pieces:
        out[seat] = jnp.where(lane >= to, roll(part[group], to - source), out[seat])
    spare = LANES - last
    end = out[-1]
    for step in range(last // spare if folds else 0):
        moved = roll(out[-1], last - spare * step)
        for i, first in folds:
            line = jnp.broadcast_to(moved[i:i + 1], (SUBLANES, LANES))
            end = jnp.where((lane >= last) & (row == first + step), line, end)
    for i in range(bins - 1):
        buffer[c, start + SUBLANES * i:start + SUBLANES * (i + 1)] = out[i]
    start += SUBLANES * (bins - 1)
    buffer[c, start:start + kept] = end[:kept]


def unpack_rest(buffer, c, start, border, tail):
    groups, bins, last, kept, pieces, folds = seats(border, tail)
    lane = lanes_of(SUBLANES)
    row = lax.broadcasted_iota(jnp.int32, (SUBLANES, LANES), 0)
    part = [buffer[c, start + SUBLANES * i:start + SUBLANES * (i + 1)] for i in range(bins - 1)]
    start += SUBLANES * (bins - 1)
    end = buffer[c, start:start + kept]
    if folds:
        end = jnp.concatenate([end, end[:SUBLANES - kept]], axis=0)
    spare = LANES - last
    whole = end
    for step in range(last // spare if folds else 0):
        moved = roll(end, spare * step - last)
        for i, first in folds:
            line = jnp.broadcast_to(moved[first + step:first + step + 1], (SUBLANES, LANES))
            whole = jnp.where((lane >= step * spare) & (row == i), line, whole)
    part.append(whole)
    for group in range(bins, groups):
        found = None
        for owner, source, seat, to in pieces:
            if owner == group:
                moved = roll(part[seat], source - to)
                found = moved if found is None else jnp.where(lane >= source, moved, found)
        part.append(found)
    return jnp.concatenate(part, axis=0)


def kernel(
    names,
    image_hbm, grad_hbm, dual_hbm, rew_hbm,
    sy0_hbm, sx0_hbm, sy1_hbm, sx1_hbm, ay0_hbm, ax0_hbm, ay1_hbm, ax1_hbm,
    next_ref, upd_ref, factor_ref,
    sy0_ref, sx0_ref, sy1_ref, sx1_ref, ay0_ref, ax0_ref, ay1_ref, ax1_ref, rew_ref,
    image, grad, dual, work, weight, y1s, y1r, las, lar, lbs, lbr, rs, rr, y2s, y2r, acc, accr,
    in_sem, const_sem, send_sem, recv_sem, side_recv, via_send, ch_send, ch_recv,
):
    fy_name, fx_name, ch_name = names
    channels, tx, ty = image.shape
    ex, ey = dual.shape[1:]
    border = ex - tx
    n = CHUNK
    chunks = channels // n
    half = ex // 2
    tail = ty - LANES
    fy, fx, ch = (lax.axis_index(a) for a in names)
    n_fy, n_fx, n_ch = (lax.axis_size(a) for a in names)
    has_up, has_down = fy > 0, fy < n_fy - 1
    has_left, has_right = fx > 0, fx < n_fx - 1

    barrier = pltpu.get_barrier_semaphore()
    near = (
        (has_up, {fy_name: fy - 1}),
        (has_down, {fy_name: fy + 1}),
        (has_left, {fx_name: fx - 1}),
        (has_right, {fx_name: fx + 1}),
        (fx > 1, {fx_name: fx - 2}),
        (fx < n_fx - 2, {fx_name: fx + 2}),
    )
    for there, where in near:
        @pl.when(there)
        def _(where=where):
            pl.semaphore_signal(barrier, inc=1, device_id=where, device_id_type=MESH)
    for step in range(1, n_ch):
        pl.semaphore_signal(
            barrier, inc=1, device_id={ch_name: lax.rem(ch + step, n_ch)}, device_id_type=MESH
        )

    def part(k):
        return pl.ds(k * n, n)

    def load(k, which):
        src, dst = ((dual_hbm, dual), (image_hbm, image), (grad_hbm, grad))[which]
        return pltpu.make_async_copy(src.at[part(k)], dst.at[part(k)], in_sem.at[which, k])

    constants = (
        (sy1_hbm, sy1_ref), (sx1_hbm, sx1_ref), (sy0_hbm, sy0_ref), (sx0_hbm, sx0_ref),
        (ay0_hbm, ay0_ref), (ax0_hbm, ax0_ref), (ay1_hbm, ay1_ref), (ax1_hbm, ax1_ref),
        (rew_hbm, rew_ref),
    )

    def constant(i):
        src, dst = constants[i]
        return pltpu.make_async_copy(src, dst, const_sem.at[i])

    corner_half, own_half = border // 2, tx // 2
    corner_rows, own_rows = pl.ds(0, corner_half), pl.ds(corner_half, own_half)
    links = (
        (y1s, y1r, {fy_name: fy - 1}, None),
        (y2s, y2r, {fy_name: fy + 1}, own_rows),
        (y2s, y2r, {fy_name: fy + 1}, corner_rows),
    )
    UP, DOWN_A, DOWN_B = range(3)
    sides = ((las, lar), (lbs, lbr), (rs, rr))
    LEFT_A, LEFT_B, RIGHT = range(3)
    HERE, PASSING = 0, 1

    def link(c, which):
        src, dst, where, rows = links[which]
        return pltpu.make_async_remote_copy(
            src_ref=src.at[c] if rows is None else src.at[c, rows],
            dst_ref=dst.at[c] if rows is None else dst.at[c, rows],
            send_sem=send_sem.at[min(which, 1)],
            recv_sem=recv_sem.at[which, c],
            device_id=where,
            device_id_type=MESH,
        )

    def link_sent(which):
        src, dst, where, _ = links[which]
        return pltpu.make_async_remote_copy(
            src_ref=src,
            dst_ref=dst,
            send_sem=send_sem.at[min(which, 1)],
            recv_sem=recv_sem.at[which, 0],
            device_id=where,
            device_id_type=MESH,
        )

    odd = lax.rem(fx, 2) == 1
    groups = n_fx // 2

    def turn(c, m):
        return ((c + 1) * m) // groups - (c * m) // groups == 1

    def sends_via(c, which):
        if which != RIGHT:
            return jnp.logical_not(odd) & has_left & has_right & turn(c, fx // 2)
        return odd & has_left & has_right & jnp.logical_not(turn(c, (fx + 1) // 2))

    def passes_on(c, which):
        if which != RIGHT:
            return odd & (fx > 2) & turn(c, fx // 2)
        return jnp.logical_not(odd) & (fx < n_fx - 2) & jnp.logical_not(turn(c, (fx + 2) // 2))

    def to_side(c, which):
        src, dst = sides[which]
        ahead, back = (fx + 1, fx - 1) if which == RIGHT else (fx - 1, fx + 1)
        around = sends_via(c, which)
        slot = jnp.where(around, PASSING, HERE)
        return pltpu.make_async_remote_copy(
            src_ref=src.at[c],
            dst_ref=dst.at[slot, c],
            send_sem=send_sem.at[2 + which],
            recv_sem=side_recv.at[which, slot, c],
            device_id={fx_name: jnp.where(around, back, ahead)},
            device_id_type=MESH,
        )

    def side_sent(which):
        src, dst = sides[which]
        return pltpu.make_async_remote_copy(
            src_ref=src,
            dst_ref=dst.at[HERE],
            send_sem=send_sem.at[2 + which],
            recv_sem=side_recv.at[which, HERE, 0],
            device_id={fx_name: fx + 1 if which == RIGHT else fx - 1},
            device_id_type=MESH,
        )

    def arrival(c, which, slot):
        src, dst = sides[which]
        return pltpu.make_async_remote_copy(
            src_ref=src.at[c],
            dst_ref=dst.at[slot, c],
            send_sem=send_sem.at[2 + which],
            recv_sem=side_recv.at[which, slot, c],
            device_id={fx_name: fx + 1 if which == RIGHT else fx - 1},
            device_id_type=MESH,
        )

    def onward(c, which):
        _, dst = sides[which]
        return pltpu.make_async_remote_copy(
            src_ref=dst.at[PASSING, c],
            dst_ref=dst.at[HERE, c],
            send_sem=via_send.at[which, c],
            recv_sem=side_recv.at[which, HERE, c],
            device_id={fx_name: fx + 2 if which == RIGHT else fx - 2},
            device_id_type=MESH,
        )

    def stage_via(ways, k):
        for j in range(n):
            c = k * n + j

            @pl.when(passes_on(c, ways[0]))
            def _(c=c):
                for way in ways:
                    arrival(c, way, PASSING).wait_recv()
                    onward(c, way).start()

    load(0, 0).start()
    for i in range(4):
        constant(i).start()

    def loads(k, carry):
        load(k, 0).start()
        return carry

    def more_loads(k, carry):
        load(k, 1).start()
        load(k, 2).start()
        return carry

    lax.fori_loop(1, chunks, loads, 0)
    lax.fori_loop(0, chunks, more_loads, 0)
    for i in range(4, 9):
        constant(i).start()
    acc[...] = jnp.zeros_like(acc)
    xs = lax.broadcasted_iota(jnp.int32, (tx, ty), 0)
    ys = lax.broadcasted_iota(jnp.int32, (tx, ty), 1)
    ax = jnp.where((xs >= tx - border) & has_right, 0.5**0.5, 1.0).astype(F32)
    by = jnp.where((ys >= ty - border) & has_down, 0.5**0.5, 1.0).astype(F32)
    weight[...] = ax * by

    peers = n_ch - 1
    for at, size in ((fy, n_fy), (fx, n_fx)):
        peers = peers + jnp.minimum(at, 1) + jnp.minimum(size - 1 - at, 1)
    peers = peers + jnp.minimum(fx // 2, 1) + jnp.minimum((n_fx - 1 - fx) // 2, 1)

    def own_edge(rows):
        at = lanes_of(rows)
        return (at >= tail - border) & (at < tail)

    half_lane = LANES // 2

    def members(k):
        return [k * n + j for j in range(n)]

    def stage_a(k):
        load(k, 0).wait()

        @pl.when(k == 0)
        def _():
            for i in range(4):
                constant(i).wait()

        x = dual[part(k)]
        hx, hy = ex // 2, ey // 2
        corner = corner_step(x[:, :hx, :hy], sy1_ref[...], sx1_ref[...])
        full = jnp.stack(
            [
                jnp.concatenate(
                    [jnp.concatenate([corner[j], x[j, :hx, hy:]], axis=1), x[j, hx:]], axis=0
                )
                for j in range(n)
            ]
        )
        mid = times_right(full, sy0_ref[...])
        for j in range(n):
            work[k * n + j] = times_left(sx0_ref[...], mid[j])

        @pl.when(k == 0)
        def _():
            pl.semaphore_wait(barrier, peers)

        @pl.when(has_up)
        def _():
            edge = own_edge(half)
            for c in members(k):
                first, second = work[c, :half, LANES:], work[c, half:, LANES:]
                y1s[c] = jnp.where(edge, roll(first, -border), roll(second, half_lane - border))
            for c in members(k):
                link(c, UP).start()

        @pl.when(has_left)
        def _():
            for c in members(k):
                las[c] = work[c, :border, :LANES]
            for c in members(k):
                to_side(c, LEFT_A).start()

    def stage_b(k):
        @pl.when(has_down)
        def _():
            for c in members(k):
                link(c, UP).wait_recv()
            edge = own_edge(half)
            for c in members(k):
                got = y1r[c]
                work[c, :half, LANES:] += jnp.where(edge, got, 0.0)
                work[c, half:, LANES:] += jnp.where(edge, roll(got, half_lane), 0.0)

        @pl.when(has_left)
        def _():
            for c in members(k):
                pack_rest(work[c, :border, LANES:], tail, lbs, c, 0)
            for c in members(k):
                to_side(c, LEFT_B).start()

    def stage_c(k):
        load(k, 1).wait()
        load(k, 2).wait()

        @pl.when(has_right)
        def _():
            for c in members(k):
                arrival(c, LEFT_A, HERE).wait_recv()
                arrival(c, LEFT_B, HERE).wait_recv()
            for c in members(k):
                work[c, ex - border:, :LANES] += lar[HERE, c]
                work[c, ex - border:, LANES:] += unpack_rest(lbr.at[HERE], c, 0, border, tail)

        for c in members(k):
            adjoint = work[c, border:, :ty] * weight[...]
            current = image[c]
            fresh = jnp.maximum(current - TAU_STEP * (grad[c].astype(F32) + adjoint), 0.0)
            work[c, border:, :ty] = (2.0 * fresh - current) * weight[...]
            next_ref[c] = fresh

        @pl.when(has_right)
        def _():
            for c in members(k):
                rs[c, :border] = work[c, ex - border:, :LANES]
                pack_rest(work[c, ex - border:, LANES:], tail, rs, c, border)
            for c in members(k):
                to_side(c, RIGHT).start()

        @pl.when(has_down)
        def _():
            mid = border + own_half
            edge = own_edge(own_half)
            for c in members(k):
                y2s[c, corner_half:] = jnp.where(
                    edge, work[c, border:mid, LANES:], roll(work[c, mid:, LANES:], half_lane)
                )
            for c in members(k):
                link(c, DOWN_A).start()

    def stage_d(k):
        @pl.when(has_left)
        def _():
            for c in members(k):
                arrival(c, RIGHT, HERE).wait_recv()
            for c in members(k):
                work[c, :border, :LANES] = rr[HERE, c, :border]
                work[c, :border, LANES:] = unpack_rest(rr.at[HERE], c, border, border, tail)

        @pl.when(jnp.logical_not(has_left))
        def _():
            for c in members(k):
                work[c, :border] = jnp.zeros((border, ey), F32)

        @pl.when(has_down)
        def _():
            edge = own_edge(corner_half)
            for c in members(k):
                y2s[c, :corner_half] = jnp.where(
                    edge,
                    work[c, :corner_half, LANES:],
                    roll(work[c, corner_half:border, LANES:], half_lane),
                )
            for c in members(k):
                link(c, DOWN_B).start()

    def stage_e(k):
        @pl.when(k == 0)
        def _():
            for i in range(4, 8):
                constant(i).wait()

        @pl.when(has_up)
        def _():
            for c in members(k):
                link(c, DOWN_A).wait_recv()
                link(c, DOWN_B).wait_recv()
            for at, rows, buffered in ((0, corner_half, 0), (border, own_half, corner_half)):
                low = lanes_of(rows) < tail
                first, second = pl.ds(at, rows), pl.ds(at + rows, rows)
                for c in members(k):
                    got = y2r[c, buffered:buffered + rows]
                    work[c, first, LANES:] = jnp.where(low, work[c, first, LANES:], roll(got, border))
                    work[c, second, LANES:] = jnp.where(
                        low, work[c, second, LANES:], roll(got, border - half_lane)
                    )

        @pl.when(jnp.logical_not(has_up))
        def _():
            low = lanes_of(ex) < tail
            for c in members(k):
                work[c, :, LANES:] = jnp.where(low, work[c, :, LANES:], 0.0)

        mid = times_right(work[part(k)], ay0_ref[...])
        hx, hy = ex // 2, ey // 2
        full = [times_left(ax0_ref[...], mid[j]) for j in range(n)]
        corner = corner_step(jnp.stack([f[:hx, :hy] for f in full]), ay1_ref[...], ax1_ref[...])
        total = acc[...]
        for j in range(n):
            c = k * n + j
            coeffs = jnp.concatenate(
                [jnp.concatenate([corner[j], full[j][:hx, hy:]], axis=1), full[j][hx:]], axis=0
            )
            updated = dual[c] + coeffs
            total = total + updated * updated
            upd_ref[c] = updated
        acc[...] = total

    stages = (
        (0, stage_a),
        (AT_B, stage_b),
        (AT_VIA_L, functools.partial(stage_via, (LEFT_A, LEFT_B))),
        (AT_VIA_R, functools.partial(stage_via, (RIGHT,))),
        (AT_C, stage_c),
        (AT_D, stage_d),
        (AT_E, stage_e),
    )

    def step(t, carry):
        for delay, stage in stages:
            @pl.when((t >= delay) & (t < chunks + delay))
            def _(delay=delay, stage=stage):
                stage(t - delay)
        return carry

    lax.fori_loop(0, chunks + AT_E, step, 0)

    def across(step):
        return pltpu.make_async_remote_copy(
            src_ref=acc,
            dst_ref=accr.at[step - 1],
            send_sem=ch_send.at[step - 1],
            recv_sem=ch_recv.at[step - 1],
            device_id={ch_name: lax.rem(ch + step, n_ch)},
            device_id_type=MESH,
        )

    for s in range(1, n_ch):
        across(s).start()
    for which, there in ((UP, has_up), (DOWN_A, has_down)):
        @pl.when(there)
        def _(which=which):
            link_sent(which).wait_send()
    for which, there in ((LEFT_A, has_left), (LEFT_B, has_left), (RIGHT, has_right)):
        @pl.when(there)
        def _(which=which):
            side_sent(which).wait_send()

    def passed(c, carry):
        for ways in ((LEFT_A, LEFT_B), (RIGHT,)):
            @pl.when(passes_on(c, ways[0]))
            def _(ways=ways):
                for way in ways:
                    onward(c, way).wait_send()
        return carry

    lax.fori_loop(0, channels, passed, 0)
    constant(8).wait()
    for s in range(1, n_ch):
        across(s).wait()
    total = acc[...]
    for s in range(1, n_ch):
        total = total + accr[s - 1]
    factor_ref[...] = jnp.minimum(1.0, LAMBDA_REG * rew_ref[...] / jnp.sqrt(total + EPSILON))


def shards(names, image_cube, data_grad, dual_coeffs, reweights):
    channels, tx, ty = image_cube.shape
    _, ex, ey = dual_coeffs.shape
    border = ex - tx
    n_ch = lax.axis_size(names[2])
    chunks = channels // CHUNK
    rest = packed_rows(border, ty - LANES)
    wy0 = np.roll(level_matrix(ey), -(ey - ty), axis=1)
    wx0 = level_matrix(ex)
    wy1, wx1 = level_matrix(ey // 2), level_matrix(ex // 2)
    px0, px1 = round_up(ex, 16), round_up(ex // 2, 16)
    factors = (
        right_factor(wy0), left_factor(wx0.T, px0), right_factor(wy1), left_factor(wx1.T, px1),
        right_factor(wy0.T), left_factor(wx0, px0), right_factor(wy1.T), left_factor(wx1, px1),
    )
    far = pl.BlockSpec(memory_space=pltpu.HBM)
    inside = pl.BlockSpec(memory_space=pltpu.VMEM)
    lines = pltpu.VMEM((channels, ex // 2, LANES), F32)
    side_rows = (border, rest, border + rest)
    side_bufs = [
        pltpu.VMEM(shape, F32)
        for rows in side_rows
        for shape in ((channels, rows, LANES), (2, channels, rows, LANES))
    ]
    operands = (image_cube, data_grad, dual_coeffs, reweights, *factors)
    image_next, updated, factor = pl.pallas_call(
        functools.partial(kernel, names),
        out_shape=(
            pltpu.VMEM((channels, tx, ty), F32),
            pltpu.VMEM((channels, ex, ey), F32),
            pltpu.VMEM((ex, ey), F32),
        ),
        in_specs=[far] * len(operands),
        out_specs=(inside,) * 3,
        scratch_shapes=[
            *(pltpu.VMEM(f.shape, f.dtype) for f in factors),
            pltpu.VMEM((ex, ey), F32),
            pltpu.VMEM((channels, tx, ty), F32),
            pltpu.VMEM((channels, tx, ty), BF16),
            pltpu.VMEM((channels, ex, ey), F32),
            pltpu.VMEM((channels, ex, ey), F32),
            pltpu.VMEM((tx, ty), F32),
            lines, lines, *side_bufs, lines, lines,
            pltpu.VMEM((ex, ey), F32),
            pltpu.VMEM((n_ch - 1, ex, ey), F32),
            pltpu.SemaphoreType.DMA((3, chunks)),
            pltpu.SemaphoreType.DMA((9,)),
            pltpu.SemaphoreType.DMA((5,)),
            pltpu.SemaphoreType.DMA((3, channels)),
            pltpu.SemaphoreType.DMA((3, 2, channels)),
            pltpu.SemaphoreType.DMA((3, channels)),
            pltpu.SemaphoreType.DMA((n_ch - 1,)),
            pltpu.SemaphoreType.DMA((n_ch - 1,)),
        ],
        compiler_params=pltpu.CompilerParams(
            collective_id=0, has_side_effects=True, vmem_limit_bytes=40 * 2**20
        ),
        name="facets",
    )(*(pltpu.with_memory_space_constraint(a, pltpu.HBM) for a in operands))
    return image_next, updated * factor[None]


def solution(mesh):
    names = ("fy", "fx", "ch")
    return jax.shard_map(
        functools.partial(shards, names),
        mesh=mesh,
        in_specs=(P("ch", "fx", "fy"), P("ch", "fx", "fy"), P("ch", "fx", "fy"), P("fx", "fy")),
        out_specs=(P("ch", "fx", "fy"), P("ch", "fx", "fy")),
        check_vma=False,
    )
```

```python
import functools

import jax
import jax.numpy as jnp
import numpy as np
from jax import lax
from jax.experimental import pallas as pl
from jax.experimental.pallas import tpu as pltpu
from jax.sharding import PartitionSpec as P

LEVELS = 2
LOW_PASS = [
    -0.00011747678400228192,
    0.0006754494059985568,
    -0.0003917403729959771,
    -0.00487035299301066,
    0.008746094047015655,
    0.013981027917015516,
    -0.04408825393106472,
    -0.01736930100202211,
    0.128747426620186,
    0.00047248457399797254,
    -0.2840155429624281,
    -0.015829105256023893,
    0.5853546836548691,
    0.6756307362980128,
    0.3128715909144659,
    0.05441584224308161,
]
TAU_STEP = 0.5
LAMBDA_REG = 1.0
EPSILON = 1e-06
LANES = 128
SUBLANES = 8
PIECES = 8
CHUNK = 4
AT_B, AT_VIA_L, AT_C, AT_VIA_R, AT_D, AT_E = 2, 3, 4, 7, 8, 9
MESH = pl.DeviceIdType.MESH
F32 = jnp.float32
BF16 = jnp.bfloat16


def level_matrix(length):
    halved = length // 2
    taps_count = len(LOW_PASS)
    matrix = np.zeros((length, length))
    for out_row in range(halved):
        for tap_index in range(taps_count):
            column = (2 * out_row + tap_index) % length
            matrix[out_row, column] += LOW_PASS[tap_index]
            matrix[halved + out_row, column] += (-1) ** tap_index * LOW_PASS[
                taps_count - 1 - tap_index
            ]
    return matrix


def halves(matrix):
    exact = np.asarray(matrix, np.float32)
    high = exact.astype(BF16)
    low = (exact - high.astype(np.float32)).astype(BF16)
    return high, low


def right_factor(matrix):
    high, low = halves(matrix)
    return jnp.asarray(np.concatenate([high, low, high], axis=0))


def left_factor(matrix, padded):
    high, low = halves(np.pad(matrix, ((0, 0), (0, padded - matrix.shape[1]))))
    return jnp.asarray(np.concatenate([high, low, high], axis=1))


def round_up(value, to):
    return -(-value // to) * to


def split(x):
    high = x.astype(BF16)
    low = (x - high.astype(F32)).astype(BF16)
    return high, low


def times_right(x, factor):
    n, rows, columns = x.shape
    high, low = split(x.reshape(n * rows, columns))
    out = jnp.dot(jnp.concatenate([high, high, low], axis=1), factor, preferred_element_type=F32)
    return out.reshape(n, rows, out.shape[1])


def times_left(factor, x):
    rows = x.shape[0]
    padded = round_up(rows, 16)
    if padded > rows:
        x = jnp.concatenate([x, jnp.zeros((padded - rows, x.shape[1]), F32)], axis=0)
    high, low = split(x)
    return jnp.dot(factor, jnp.concatenate([high, high, low], axis=0), preferred_element_type=F32)


def corner_step(corner, right, left):
    n = corner.shape[0]
    width = corner.shape[2]
    mid = times_right(corner, right)
    pieces = []
    for c in range(0, n, 2):
        pair = times_left(left, jnp.concatenate([mid[c], mid[c + 1]], axis=1))
        pieces += [pair[:, :width], pair[:, width:]]
    return pieces


def lanes_of(rows):
    return lax.broadcasted_iota(jnp.int32, (rows, LANES), 1)


def roll(x, by):
    return pltpu.roll(x, by % LANES, 1)


def seats(border, tail):
    groups = border // SUBLANES
    bins = -(-groups * tail // LANES)
    last = groups * tail - (bins - 1) * LANES
    pieces, seat, at = [], 0, tail
    for group in range(bins, groups):
        lane = 0
        while lane < tail:
            room = LANES if seat < bins - 1 else last
            if at == room:
                seat, at = seat + 1, tail
                continue
            width = min(tail - lane, room - at)
            pieces.append((group, lane, seat, at))
            lane, at = lane + width, at + width
    spare = LANES - last
    kept = SUBLANES * last // LANES
    folds = []
    if spare:
        assert last % spare == 0 and (SUBLANES - kept) * last == spare * kept
        folds = [(row, (row - kept) * (last // spare)) for row in range(kept, SUBLANES)]
    return groups, bins, last, kept, pieces, folds


def packed_rows(border, tail):
    _, bins, _, kept, _, _ = seats(border, tail)
    return (bins - 1) * SUBLANES + kept


def pack_rest(rest, tail, buffer, c, start):
    groups, bins, last, kept, pieces, folds = seats(rest.shape[0], tail)
    lane = lanes_of(SUBLANES)
    row = lax.broadcasted_iota(jnp.int32, (SUBLANES, LANES), 0)
    part = [rest[SUBLANES * i:SUBLANES * (i + 1)] for i in range(groups)]
    out = part[:bins]
    for group, source, seat, to in pieces:
        out[seat] = jnp.where(lane >= to, roll(part[group], to - source), out[seat])
    spare = LANES - last
    end = out[-1]
    for step in range(last // spare if folds else 0):
        moved = roll(out[-1], last - spare * step)
        for i, first in folds:
            line = jnp.broadcast_to(moved[i:i + 1], (SUBLANES, LANES))
            end = jnp.where((lane >= last) & (row == first + step), line, end)
    for i in range(bins - 1):
        buffer[c, start + SUBLANES * i:start + SUBLANES * (i + 1)] = out[i]
    start += SUBLANES * (bins - 1)
    buffer[c, start:start + kept] = end[:kept]


def unpack_rest(buffer, c, start, border, tail):
    groups, bins, last, kept, pieces, folds = seats(border, tail)
    lane = lanes_of(SUBLANES)
    row = lax.broadcasted_iota(jnp.int32, (SUBLANES, LANES), 0)
    part = [buffer[c, start + SUBLANES * i:start + SUBLANES * (i + 1)] for i in range(bins - 1)]
    start += SUBLANES * (bins - 1)
    end = buffer[c, start:start + kept]
    if folds:
        end = jnp.concatenate([end, end[:SUBLANES - kept]], axis=0)
    spare = LANES - last
    whole = end
    for step in range(last // spare if folds else 0):
        moved = roll(end, spare * step - last)
        for i, first in folds:
            line = jnp.broadcast_to(moved[first + step:first + step + 1], (SUBLANES, LANES))
            whole = jnp.where((lane >= step * spare) & (row == i), line, whole)
    part.append(whole)
    for group in range(bins, groups):
        found = None
        for owner, source, seat, to in pieces:
            if owner == group:
                moved = roll(part[seat], source - to)
                found = moved if found is None else jnp.where(lane >= source, moved, found)
        part.append(found)
    return jnp.concatenate(part, axis=0)


def kernel(
    names,
    image_hbm, grad_hbm, dual_hbm, rew_hbm,
    sy0_hbm, sx0_hbm, sy1_hbm, sx1_hbm, ay0_hbm, ax0_hbm, ay1_hbm, ax1_hbm,
    next_ref, upd_ref, factor_ref,
    sy0_ref, sx0_ref, sy1_ref, sx1_ref, ay0_ref, ax0_ref, ay1_ref, ax1_ref, rew_ref,
    image, grad, dual, work, weight, y1s, y1r, las, lar, lbs, lbr, rs, rr, y2s, y2r, acc, accr,
    in_sem, const_sem, send_sem, recv_sem, side_recv, via_send, ch_send, ch_recv,
):
    fy_name, fx_name, ch_name = names
    channels, tx, ty = image.shape
    ex, ey = dual.shape[1:]
    border = ex - tx
    n = CHUNK
    chunks = channels // n
    half = ex // 2
    tail = ty - LANES
    fy, fx, ch = (lax.axis_index(a) for a in names)
    n_fy, n_fx, n_ch = (lax.axis_size(a) for a in names)
    has_up, has_down = fy > 0, fy < n_fy - 1
    has_left, has_right = fx > 0, fx < n_fx - 1

    barrier = pltpu.get_barrier_semaphore()
    near = (
        (has_up, {fy_name: fy - 1}),
        (has_down, {fy_name: fy + 1}),
        (has_left, {fx_name: fx - 1}),
        (has_right, {fx_name: fx + 1}),
        (fx > 1, {fx_name: fx - 2}),
        (fx < n_fx - 2, {fx_name: fx + 2}),
    )
    for there, where in near:
        @pl.when(there)
        def _(where=where):
            pl.semaphore_signal(barrier, inc=1, device_id=where, device_id_type=MESH)
    for step in range(1, n_ch):
        pl.semaphore_signal(
            barrier, inc=1, device_id={ch_name: lax.rem(ch + step, n_ch)}, device_id_type=MESH
        )

    def part(k):
        return pl.ds(k * n, n)

    def load(k, which):
        src, dst = ((dual_hbm, dual), (image_hbm, image), (grad_hbm, grad))[which]
        return pltpu.make_async_copy(src.at[part(k)], dst.at[part(k)], in_sem.at[which, k])

    constants = (
        (sy1_hbm, sy1_ref), (sx1_hbm, sx1_ref), (sy0_hbm, sy0_ref), (sx0_hbm, sx0_ref),
        (ay0_hbm, ay0_ref), (ax0_hbm, ax0_ref), (ay1_hbm, ay1_ref), (ax1_hbm, ax1_ref),
        (rew_hbm, rew_ref),
    )

    def constant(i):
        src, dst = constants[i]
        return pltpu.make_async_copy(src, dst, const_sem.at[i])

    corner_half, own_half = border // 2, tx // 2
    corner_rows, own_rows = pl.ds(0, corner_half), pl.ds(corner_half, own_half)
    links = (
        (y1s, y1r, {fy_name: fy - 1}, None),
        (y2s, y2r, {fy_name: fy + 1}, own_rows),
        (y2s, y2r, {fy_name: fy + 1}, corner_rows),
    )
    UP, DOWN_A, DOWN_B = range(3)
    sides = ((las, lar), (lbs, lbr), (rs, rr))
    LEFT_A, LEFT_B, RIGHT = range(3)
    HERE, PASSING = 0, 1

    def link(c, which):
        src, dst, where, rows = links[which]
        return pltpu.make_async_remote_copy(
            src_ref=src.at[c] if rows is None else src.at[c, rows],
            dst_ref=dst.at[c] if rows is None else dst.at[c, rows],
            send_sem=send_sem.at[min(which, 1)],
            recv_sem=recv_sem.at[which, c],
            device_id=where,
            device_id_type=MESH,
        )

    def link_sent(which):
        src, dst, where, _ = links[which]
        return pltpu.make_async_remote_copy(
            src_ref=src,
            dst_ref=dst,
            send_sem=send_sem.at[min(which, 1)],
            recv_sem=recv_sem.at[which, 0],
            device_id=where,
            device_id_type=MESH,
        )

    odd = lax.rem(fx, 2) == 1
    groups = n_fx // 2

    def turn(c, m):
        return ((c + 1) * m) // groups - (c * m) // groups == 1

    def sends_via(c, which):
        if which != RIGHT:
            return jnp.logical_not(odd) & has_left & has_right & turn(c, fx // 2)
        return odd & has_left & has_right & jnp.logical_not(turn(c, (fx + 1) // 2))

    def passes_on(c, which):
        if which != RIGHT:
            return odd & (fx > 2) & turn(c, fx // 2)
        return jnp.logical_not(odd) & (fx < n_fx - 2) & jnp.logical_not(turn(c, (fx + 2) // 2))

    def to_side(c, which):
        src, dst = sides[which]
        ahead, back = (fx + 1, fx - 1) if which == RIGHT else (fx - 1, fx + 1)
        around = sends_via(c, which)
        slot = jnp.where(around, PASSING, HERE)
        return pltpu.make_async_remote_copy(
            src_ref=src.at[c],
            dst_ref=dst.at[slot, c],
            send_sem=send_sem.at[2 + which],
            recv_sem=side_recv.at[which, slot, c],
            device_id={fx_name: jnp.where(around, back, ahead)},
            device_id_type=MESH,
        )

    def side_sent(which):
        src, dst = sides[which]
        return pltpu.make_async_remote_copy(
            src_ref=src,
            dst_ref=dst.at[HERE],
            send_sem=send_sem.at[2 + which],
            recv_sem=side_recv.at[which, HERE, 0],
            device_id={fx_name: fx + 1 if which == RIGHT else fx - 1},
            device_id_type=MESH,
        )

    def arrival(c, which, slot):
        src, dst = sides[which]
        return pltpu.make_async_remote_copy(
            src_ref=src.at[c],
            dst_ref=dst.at[slot, c],
            send_sem=send_sem.at[2 + which],
            recv_sem=side_recv.at[which, slot, c],
            device_id={fx_name: fx + 1 if which == RIGHT else fx - 1},
            device_id_type=MESH,
        )

    def onward(c, which):
        _, dst = sides[which]
        return pltpu.make_async_remote_copy(
            src_ref=dst.at[PASSING, c],
            dst_ref=dst.at[HERE, c],
            send_sem=via_send.at[which, c],
            recv_sem=side_recv.at[which, HERE, c],
            device_id={fx_name: fx + 2 if which == RIGHT else fx - 2},
            device_id_type=MESH,
        )

    def stage_via(ways, k):
        for j in range(n):
            c = k * n + j

            @pl.when(passes_on(c, ways[0]))
            def _(c=c):
                for way in ways:
                    arrival(c, way, PASSING).wait_recv()
                    onward(c, way).start()

    load(0, 0).start()
    for i in range(4):
        constant(i).start()

    def loads(k, carry):
        load(k, 0).start()
        return carry

    def more_loads(k, carry):
        load(k, 1).start()
        load(k, 2).start()
        return carry

    lax.fori_loop(1, chunks, loads, 0)
    lax.fori_loop(0, chunks, more_loads, 0)
    for i in range(4, 9):
        constant(i).start()
    acc[...] = jnp.zeros_like(acc)
    xs = lax.broadcasted_iota(jnp.int32, (tx, ty), 0)
    ys = lax.broadcasted_iota(jnp.int32, (tx, ty), 1)
    ax = jnp.where((xs >= tx - border) & has_right, 0.5**0.5, 1.0).astype(F32)
    by = jnp.where((ys >= ty - border) & has_down, 0.5**0.5, 1.0).astype(F32)
    weight[...] = ax * by

    peers = n_ch - 1
    for at, size in ((fy, n_fy), (fx, n_fx)):
        peers = peers + jnp.minimum(at, 1) + jnp.minimum(size - 1 - at, 1)
    peers = peers + jnp.minimum(fx // 2, 1) + jnp.minimum((n_fx - 1 - fx) // 2, 1)

    def own_edge(rows):
        at = lanes_of(rows)
        return (at >= tail - border) & (at < tail)

    half_lane = LANES // 2

    def members(k):
        return [k * n + j for j in range(n)]

    def stage_a(k, first=False):
        load(k, 0).wait()

        if first:
            for i in range(4):
                constant(i).wait()

        x = dual[part(k)]
        hx, hy = ex // 2, ey // 2
        corner = corner_step(x[:, :hx, :hy], sy1_ref[...], sx1_ref[...])
        full = jnp.stack(
            [
                jnp.concatenate(
                    [jnp.concatenate([corner[j], x[j, :hx, hy:]], axis=1), x[j, hx:]], axis=0
                )
                for j in range(n)
            ]
        )
        mid = times_right(full, sy0_ref[...])
        for j in range(n):
            work[k * n + j] = times_left(sx0_ref[...], mid[j])

        if first:
            pl.semaphore_wait(barrier, peers)

        @pl.when(has_up)
        def _():
            edge = own_edge(half)
            for c in members(k):
                first, second = work[c, :half, LANES:], work[c, half:, LANES:]
                y1s[c] = jnp.where(edge, roll(first, -border), roll(second, half_lane - border))
            for c in members(k):
                link(c, UP).start()

        @pl.when(has_left)
        def _():
            for c in members(k):
                las[c] = work[c, :border, :LANES]
            for c in members(k):
                to_side(c, LEFT_A).start()

    def stage_b(k):
        @pl.when(has_down)
        def _():
            for c in members(k):
                link(c, UP).wait_recv()
            edge = own_edge(half)
            for c in members(k):
                got = y1r[c]
                work[c, :half, LANES:] += jnp.where(edge, got, 0.0)
                work[c, half:, LANES:] += jnp.where(edge, roll(got, half_lane), 0.0)

        @pl.when(has_left)
        def _():
            for c in members(k):
                pack_rest(work[c, :border, LANES:], tail, lbs, c, 0)
            for c in members(k):
                to_side(c, LEFT_B).start()

    def stage_c(k):
        load(k, 1).wait()
        load(k, 2).wait()

        @pl.when(has_right)
        def _():
            for c in members(k):
                arrival(c, LEFT_A, HERE).wait_recv()
                arrival(c, LEFT_B, HERE).wait_recv()
            for c in members(k):
                work[c, ex - border:, :LANES] += lar[HERE, c]
                work[c, ex - border:, LANES:] += unpack_rest(lbr.at[HERE], c, 0, border, tail)

        for c in members(k):
            adjoint = work[c, border:, :ty] * weight[...]
            current = image[c]
            fresh = jnp.maximum(current - TAU_STEP * (grad[c].astype(F32) + adjoint), 0.0)
            work[c, border:, :ty] = (2.0 * fresh - current) * weight[...]
            next_ref[c] = fresh

        @pl.when(has_right)
        def _():
            for c in members(k):
                rs[c, :border] = work[c, ex - border:, :LANES]
                pack_rest(work[c, ex - border:, LANES:], tail, rs, c, border)
            for c in members(k):
                to_side(c, RIGHT).start()

        @pl.when(has_down)
        def _():
            mid = border + own_half
            edge = own_edge(own_half)
            for c in members(k):
                y2s[c, corner_half:] = jnp.where(
                    edge, work[c, border:mid, LANES:], roll(work[c, mid:, LANES:], half_lane)
                )
            for c in members(k):
                link(c, DOWN_A).start()

    def stage_d(k):
        @pl.when(has_left)
        def _():
            for c in members(k):
                arrival(c, RIGHT, HERE).wait_recv()
            for c in members(k):
                work[c, :border, :LANES] = rr[HERE, c, :border]
                work[c, :border, LANES:] = unpack_rest(rr.at[HERE], c, border, border, tail)

        @pl.when(jnp.logical_not(has_left))
        def _():
            for c in members(k):
                work[c, :border] = jnp.zeros((border, ey), F32)

        @pl.when(has_down)
        def _():
            edge = own_edge(corner_half)
            for c in members(k):
                y2s[c, :corner_half] = jnp.where(
                    edge,
                    work[c, :corner_half, LANES:],
                    roll(work[c, corner_half:border, LANES:], half_lane),
                )
            for c in members(k):
                link(c, DOWN_B).start()

    def stage_e(k):
        @pl.when(k == 0)
        def _():
            for i in range(4, 8):
                constant(i).wait()

        @pl.when(has_up)
        def _():
            for c in members(k):
                link(c, DOWN_A).wait_recv()
                link(c, DOWN_B).wait_recv()
            for at, rows, buffered in ((0, corner_half, 0), (border, own_half, corner_half)):
                low = lanes_of(rows) < tail
                first, second = pl.ds(at, rows), pl.ds(at + rows, rows)
                for c in members(k):
                    got = y2r[c, buffered:buffered + rows]
                    work[c, first, LANES:] = jnp.where(low, work[c, first, LANES:], roll(got, border))
                    work[c, second, LANES:] = jnp.where(
                        low, work[c, second, LANES:], roll(got, border - half_lane)
                    )

        @pl.when(jnp.logical_not(has_up))
        def _():
            low = lanes_of(ex) < tail
            for c in members(k):
                work[c, :, LANES:] = jnp.where(low, work[c, :, LANES:], 0.0)

        mid = times_right(work[part(k)], ay0_ref[...])
        hx, hy = ex // 2, ey // 2
        full = [times_left(ax0_ref[...], mid[j]) for j in range(n)]
        corner = corner_step(jnp.stack([f[:hx, :hy] for f in full]), ay1_ref[...], ax1_ref[...])
        total = acc[...]
        for j in range(n):
            c = k * n + j
            coeffs = jnp.concatenate(
                [jnp.concatenate([corner[j], full[j][:hx, hy:]], axis=1), full[j][hx:]], axis=0
            )
            updated = dual[c] + coeffs
            total = total + updated * updated
            upd_ref[c] = updated
        acc[...] = total

    stages = (
        (0, stage_a),
        (1, stage_b),
        (2, functools.partial(stage_via, (LEFT_A, LEFT_B))),
        (3, stage_c),
        (4, functools.partial(stage_via, (RIGHT,))),
        (5, stage_d),
        (6, stage_e),
    )

    stage_a(0, True)

    def step(t, carry):
        for delay, stage in stages:
            early = 1 if stage is stage_a else 0

            @pl.when((t >= delay + early) & (t < chunks + delay))
            def _(delay=delay, stage=stage):
                stage(t - delay)
        return carry

    lax.fori_loop(0, chunks + 6, step, 0)

    def across(step):
        return pltpu.make_async_remote_copy(
            src_ref=acc,
            dst_ref=accr.at[step - 1],
            send_sem=ch_send.at[step - 1],
            recv_sem=ch_recv.at[step - 1],
            device_id={ch_name: lax.rem(ch + step, n_ch)},
            device_id_type=MESH,
        )

    for s in range(1, n_ch):
        across(s).start()
    for which, there in ((UP, has_up), (DOWN_A, has_down)):
        @pl.when(there)
        def _(which=which):
            link_sent(which).wait_send()
    for which, there in ((LEFT_A, has_left), (LEFT_B, has_left), (RIGHT, has_right)):
        @pl.when(there)
        def _(which=which):
            side_sent(which).wait_send()

    def passed(c, carry):
        for ways in ((LEFT_A, LEFT_B), (RIGHT,)):
            @pl.when(passes_on(c, ways[0]))
            def _(ways=ways):
                for way in ways:
                    onward(c, way).wait_send()
        return carry

    lax.fori_loop(0, channels, passed, 0)
    constant(8).wait()
    for s in range(1, n_ch):
        across(s).wait()
    total = acc[...]
    for s in range(1, n_ch):
        total = total + accr[s - 1]
    factor_ref[...] = jnp.minimum(1.0, LAMBDA_REG * rew_ref[...] / jnp.sqrt(total + EPSILON))


def finish(image_ref, upd_ref, factor_ref, next_hbm, dual_hbm, scaled, sem):
    channels = upd_ref.shape[0]
    n = channels // PIECES

    def image_out(i):
        at = pl.ds(i * n, n)
        return pltpu.make_async_copy(image_ref.at[at], next_hbm.at[at], sem.at[0, i])

    def dual_out(i):
        at = pl.ds(i * n, n)
        return pltpu.make_async_copy(scaled.at[at], dual_hbm.at[at], sem.at[1, i])

    for i in range(PIECES):
        image_out(i).start()

    def piece(i, carry):
        for j in range(n):
            scaled[i * n + j] = upd_ref[i * n + j] * factor_ref[...]
        dual_out(i).start()
        return carry

    lax.fori_loop(0, PIECES, piece, 0)
    for i in range(PIECES):
        image_out(i).wait()
        dual_out(i).wait()


def shards(names, image_cube, data_grad, dual_coeffs, reweights):
    channels, tx, ty = image_cube.shape
    _, ex, ey = dual_coeffs.shape
    border = ex - tx
    n_ch = lax.axis_size(names[2])
    chunks = channels // CHUNK
    rest = packed_rows(border, ty - LANES)
    wy0 = np.roll(level_matrix(ey), -(ey - ty), axis=1)
    wx0 = level_matrix(ex)
    wy1, wx1 = level_matrix(ey // 2), level_matrix(ex // 2)
    px0, px1 = round_up(ex, 16), round_up(ex // 2, 16)
    factors = (
        right_factor(wy0), left_factor(wx0.T, px0), right_factor(wy1), left_factor(wx1.T, px1),
        right_factor(wy0.T), left_factor(wx0, px0), right_factor(wy1.T), left_factor(wx1, px1),
    )
    far = pl.BlockSpec(memory_space=pltpu.HBM)
    inside = pl.BlockSpec(memory_space=pltpu.VMEM)
    lines = pltpu.VMEM((channels, ex // 2, LANES), F32)
    side_rows = (border, rest, border + rest)
    side_bufs = [
        pltpu.VMEM(shape, F32)
        for rows in side_rows
        for shape in ((channels, rows, LANES), (2, channels, rows, LANES))
    ]
    operands = (image_cube, data_grad, dual_coeffs, reweights, *factors)
    image_next, updated, factor = pl.pallas_call(
        functools.partial(kernel, names),
        out_shape=(
            pltpu.VMEM((channels, tx, ty), F32),
            pltpu.VMEM((channels, ex, ey), F32),
            pltpu.VMEM((ex, ey), F32),
        ),
        in_specs=[far] * len(operands),
        out_specs=(inside,) * 3,
        scratch_shapes=[
            *(pltpu.VMEM(f.shape, f.dtype) for f in factors),
            pltpu.VMEM((ex, ey), F32),
            pltpu.VMEM((channels, tx, ty), F32),
            pltpu.VMEM((channels, tx, ty), BF16),
            pltpu.VMEM((channels, ex, ey), F32),
            pltpu.VMEM((channels, ex, ey), F32),
            pltpu.VMEM((tx, ty), F32),
            lines, lines, *side_bufs, lines, lines,
            pltpu.VMEM((ex, ey), F32),
            pltpu.VMEM((n_ch - 1, ex, ey), F32),
            pltpu.SemaphoreType.DMA((3, chunks)),
            pltpu.SemaphoreType.DMA((9,)),
            pltpu.SemaphoreType.DMA((5,)),
            pltpu.SemaphoreType.DMA((3, channels)),
            pltpu.SemaphoreType.DMA((3, 2, channels)),
            pltpu.SemaphoreType.DMA((3, channels)),
            pltpu.SemaphoreType.DMA((n_ch - 1,)),
            pltpu.SemaphoreType.DMA((n_ch - 1,)),
        ],
        compiler_params=pltpu.CompilerParams(
            collective_id=0, has_side_effects=True, vmem_limit_bytes=40 * 2**20
        ),
        name="facets",
    )(*(pltpu.with_memory_space_constraint(a, pltpu.HBM) for a in operands))
    anywhere = pl.BlockSpec(memory_space=pl.ANY)
    return pl.pallas_call(
        finish,
        out_shape=(
            jax.ShapeDtypeStruct((channels, tx, ty), F32),
            jax.ShapeDtypeStruct((channels, ex, ey), F32),
        ),
        in_specs=[inside] * 3,
        out_specs=(anywhere, anywhere),
        scratch_shapes=[
            pltpu.VMEM((channels, ex, ey), F32),
            pltpu.SemaphoreType.DMA((2, PIECES)),
        ],
        compiler_params=pltpu.CompilerParams(vmem_limit_bytes=40 * 2**20),
        name="finish",
    )(*(pltpu.with_memory_space_constraint(a, pltpu.VMEM) for a in (image_next, updated, factor)))


def solution(mesh):
    names = ("fy", "fx", "ch")
    return jax.shard_map(
        functools.partial(shards, names),
        mesh=mesh,
        in_specs=(P("ch", "fx", "fy"), P("ch", "fx", "fy"), P("ch", "fx", "fy"), P("fx", "fy")),
        out_specs=(P("ch", "fx", "fy"), P("ch", "fx", "fy")),
        check_vma=False,
    )
```

```python
import functools

import jax
import jax.numpy as jnp
import numpy as np
from jax import lax
from jax.experimental import pallas as pl
from jax.experimental.pallas import tpu as pltpu
from jax.sharding import PartitionSpec as P

LEVELS = 2
LOW_PASS = [
    -0.00011747678400228192,
    0.0006754494059985568,
    -0.0003917403729959771,
    -0.00487035299301066,
    0.008746094047015655,
    0.013981027917015516,
    -0.04408825393106472,
    -0.01736930100202211,
    0.128747426620186,
    0.00047248457399797254,
    -0.2840155429624281,
    -0.015829105256023893,
    0.5853546836548691,
    0.6756307362980128,
    0.3128715909144659,
    0.05441584224308161,
]
TAU_STEP = 0.5
LAMBDA_REG = 1.0
EPSILON = 1e-06
LANES = 128
SUBLANES = 8
PIECES = 8
SUB = 2
CHUNK = 4
AT_B, AT_VIA_L, AT_C, AT_VIA_R, AT_D, AT_E = 2, 3, 4, 7, 8, 9
MESH = pl.DeviceIdType.MESH
F32 = jnp.float32
BF16 = jnp.bfloat16


def level_matrix(length):
    halved = length // 2
    taps_count = len(LOW_PASS)
    matrix = np.zeros((length, length))
    for out_row in range(halved):
        for tap_index in range(taps_count):
            column = (2 * out_row + tap_index) % length
            matrix[out_row, column] += LOW_PASS[tap_index]
            matrix[halved + out_row, column] += (-1) ** tap_index * LOW_PASS[
                taps_count - 1 - tap_index
            ]
    return matrix


def halves(matrix):
    exact = np.asarray(matrix, np.float32)
    high = exact.astype(BF16)
    low = (exact - high.astype(np.float32)).astype(BF16)
    return high, low


def right_factor(matrix):
    high, low = halves(matrix)
    return jnp.asarray(np.concatenate([high, low, high], axis=0))


def left_factor(matrix, padded):
    high, low = halves(np.pad(matrix, ((0, 0), (0, padded - matrix.shape[1]))))
    return jnp.asarray(np.concatenate([high, low, high], axis=1))


def round_up(value, to):
    return -(-value // to) * to


def split(x):
    high = x.astype(BF16)
    low = (x - high.astype(F32)).astype(BF16)
    return high, low


def times_right(x, factor):
    n, rows, columns = x.shape
    high, low = split(x.reshape(n * rows, columns))
    out = jnp.dot(jnp.concatenate([high, high, low], axis=1), factor, preferred_element_type=F32)
    return out.reshape(n, rows, out.shape[1])


def times_left(factor, x):
    rows = x.shape[0]
    padded = round_up(rows, 16)
    if padded > rows:
        x = jnp.concatenate([x, jnp.zeros((padded - rows, x.shape[1]), F32)], axis=0)
    high, low = split(x)
    return jnp.dot(factor, jnp.concatenate([high, high, low], axis=0), preferred_element_type=F32)


def corner_step(corner, right, left):
    n = corner.shape[0]
    width = corner.shape[2]
    mid = times_right(corner, right)
    pieces = []
    for c in range(0, n, 2):
        pair = times_left(left, jnp.concatenate([mid[c], mid[c + 1]], axis=1))
        pieces += [pair[:, :width], pair[:, width:]]
    return pieces


def lanes_of(rows):
    return lax.broadcasted_iota(jnp.int32, (rows, LANES), 1)


def roll(x, by):
    return pltpu.roll(x, by % LANES, 1)


def seats(border, tail):
    groups = border // SUBLANES
    bins = -(-groups * tail // LANES)
    last = groups * tail - (bins - 1) * LANES
    pieces, seat, at = [], 0, tail
    for group in range(bins, groups):
        lane = 0
        while lane < tail:
            room = LANES if seat < bins - 1 else last
            if at == room:
                seat, at = seat + 1, tail
                continue
            width = min(tail - lane, room - at)
            pieces.append((group, lane, seat, at))
            lane, at = lane + width, at + width
    spare = LANES - last
    kept = SUBLANES * last // LANES
    folds = []
    if spare:
        assert last % spare == 0 and (SUBLANES - kept) * last == spare * kept
        folds = [(row, (row - kept) * (last // spare)) for row in range(kept, SUBLANES)]
    return groups, bins, last, kept, pieces, folds


def packed_rows(border, tail):
    _, bins, _, kept, _, _ = seats(border, tail)
    return (bins - 1) * SUBLANES + kept


def pack_rest(rest, tail, buffer, c, start):
    groups, bins, last, kept, pieces, folds = seats(rest.shape[0], tail)
    lane = lanes_of(SUBLANES)
    row = lax.broadcasted_iota(jnp.int32, (SUBLANES, LANES), 0)
    part = [rest[SUBLANES * i:SUBLANES * (i + 1)] for i in range(groups)]
    out = part[:bins]
    for group, source, seat, to in pieces:
        out[seat] = jnp.where(lane >= to, roll(part[group], to - source), out[seat])
    spare = LANES - last
    end = out[-1]
    for step in range(last // spare if folds else 0):
        moved = roll(out[-1], last - spare * step)
        for i, first in folds:
            line = jnp.broadcast_to(moved[i:i + 1], (SUBLANES, LANES))
            end = jnp.where((lane >= last) & (row == first + step), line, end)
    for i in range(bins - 1):
        buffer[c, start + SUBLANES * i:start + SUBLANES * (i + 1)] = out[i]
    start += SUBLANES * (bins - 1)
    buffer[c, start:start + kept] = end[:kept]


def unpack_rest(buffer, c, start, border, tail):
    groups, bins, last, kept, pieces, folds = seats(border, tail)
    lane = lanes_of(SUBLANES)
    row = lax.broadcasted_iota(jnp.int32, (SUBLANES, LANES), 0)
    part = [buffer[c, start + SUBLANES * i:start + SUBLANES * (i + 1)] for i in range(bins - 1)]
    start += SUBLANES * (bins - 1)
    end = buffer[c, start:start + kept]
    if folds:
        end = jnp.concatenate([end, end[:SUBLANES - kept]], axis=0)
    spare = LANES - last
    whole = end
    for step in range(last // spare if folds else 0):
        moved = roll(end, spare * step - last)
        for i, first in folds:
            line = jnp.broadcast_to(moved[first + step:first + step + 1], (SUBLANES, LANES))
            whole = jnp.where((lane >= step * spare) & (row == i), line, whole)
    part.append(whole)
    for group in range(bins, groups):
        found = None
        for owner, source, seat, to in pieces:
            if owner == group:
                moved = roll(part[seat], source - to)
                found = moved if found is None else jnp.where(lane >= source, moved, found)
        part.append(found)
    return jnp.concatenate(part, axis=0)


def kernel(
    names,
    image_hbm, grad_hbm, dual_hbm, rew_hbm,
    sy0_hbm, sx0_hbm, sy1_hbm, sx1_hbm, ay0_hbm, ax0_hbm, ay1_hbm, ax1_hbm,
    next_ref, upd_ref, factor_ref,
    sy0_ref, sx0_ref, sy1_ref, sx1_ref, ay0_ref, ax0_ref, ay1_ref, ax1_ref, rew_ref,
    image, grad, dual, work, weight, y1s, y1r, las, lar, lbs, lbr, rs, rr, y2s, y2r, acc, accr,
    in_sem, const_sem, send_sem, recv_sem, side_recv, via_send, ch_send, ch_recv,
):
    fy_name, fx_name, ch_name = names
    channels, tx, ty = image.shape
    ex, ey = dual.shape[1:]
    border = ex - tx
    n = CHUNK
    chunks = channels // n
    half = ex // 2
    tail = ty - LANES
    fy, fx, ch = (lax.axis_index(a) for a in names)
    n_fy, n_fx, n_ch = (lax.axis_size(a) for a in names)
    has_up, has_down = fy > 0, fy < n_fy - 1
    has_left, has_right = fx > 0, fx < n_fx - 1

    barrier = pltpu.get_barrier_semaphore()
    near = (
        (has_up, {fy_name: fy - 1}),
        (has_down, {fy_name: fy + 1}),
        (has_left, {fx_name: fx - 1}),
        (has_right, {fx_name: fx + 1}),
        (fx > 1, {fx_name: fx - 2}),
        (fx < n_fx - 2, {fx_name: fx + 2}),
    )
    for there, where in near:
        @pl.when(there)
        def _(where=where):
            pl.semaphore_signal(barrier, inc=1, device_id=where, device_id_type=MESH)
    for step in range(1, n_ch):
        pl.semaphore_signal(
            barrier, inc=1, device_id={ch_name: lax.rem(ch + step, n_ch)}, device_id_type=MESH
        )

    def part(k):
        return pl.ds(k * n, n)

    def load(k, which):
        src, dst = ((dual_hbm, dual), (image_hbm, image), (grad_hbm, grad))[which]
        return pltpu.make_async_copy(src.at[part(k)], dst.at[part(k)], in_sem.at[which, k])

    constants = (
        (sy1_hbm, sy1_ref), (sx1_hbm, sx1_ref), (sy0_hbm, sy0_ref), (sx0_hbm, sx0_ref),
        (ay0_hbm, ay0_ref), (ax0_hbm, ax0_ref), (ay1_hbm, ay1_ref), (ax1_hbm, ax1_ref),
        (rew_hbm, rew_ref),
    )

    def constant(i):
        src, dst = constants[i]
        return pltpu.make_async_copy(src, dst, const_sem.at[i])

    corner_half, own_half = border // 2, tx // 2
    corner_rows, own_rows = pl.ds(0, corner_half), pl.ds(corner_half, own_half)
    links = (
        (y1s, y1r, {fy_name: fy - 1}, None),
        (y2s, y2r, {fy_name: fy + 1}, own_rows),
        (y2s, y2r, {fy_name: fy + 1}, corner_rows),
    )
    UP, DOWN_A, DOWN_B = range(3)
    sides = ((las, lar), (lbs, lbr), (rs, rr))
    LEFT_A, LEFT_B, RIGHT = range(3)
    HERE, PASSING = 0, 1

    def link(c, which):
        src, dst, where, rows = links[which]
        return pltpu.make_async_remote_copy(
            src_ref=src.at[c] if rows is None else src.at[c, rows],
            dst_ref=dst.at[c] if rows is None else dst.at[c, rows],
            send_sem=send_sem.at[min(which, 1)],
            recv_sem=recv_sem.at[which, c],
            device_id=where,
            device_id_type=MESH,
        )

    def link_sent(which):
        src, dst, where, _ = links[which]
        return pltpu.make_async_remote_copy(
            src_ref=src,
            dst_ref=dst,
            send_sem=send_sem.at[min(which, 1)],
            recv_sem=recv_sem.at[which, 0],
            device_id=where,
            device_id_type=MESH,
        )

    odd = lax.rem(fx, 2) == 1
    groups = n_fx // 2

    def turn(c, m):
        return ((c + 1) * m) // groups - (c * m) // groups == 1

    def sends_via(c, which):
        if which != RIGHT:
            return jnp.logical_not(odd) & has_left & has_right & turn(c, fx // 2)
        return odd & has_left & has_right & jnp.logical_not(turn(c, (fx + 1) // 2))

    def passes_on(c, which):
        if which != RIGHT:
            return odd & (fx > 2) & turn(c, fx // 2)
        return jnp.logical_not(odd) & (fx < n_fx - 2) & jnp.logical_not(turn(c, (fx + 2) // 2))

    def to_side(c, which):
        src, dst = sides[which]
        ahead, back = (fx + 1, fx - 1) if which == RIGHT else (fx - 1, fx + 1)
        around = sends_via(c, which)
        slot = jnp.where(around, PASSING, HERE)
        return pltpu.make_async_remote_copy(
            src_ref=src.at[c],
            dst_ref=dst.at[slot, c],
            send_sem=send_sem.at[2 + which],
            recv_sem=side_recv.at[which, slot, c],
            device_id={fx_name: jnp.where(around, back, ahead)},
            device_id_type=MESH,
        )

    def side_sent(which):
        src, dst = sides[which]
        return pltpu.make_async_remote_copy(
            src_ref=src,
            dst_ref=dst.at[HERE],
            send_sem=send_sem.at[2 + which],
            recv_sem=side_recv.at[which, HERE, 0],
            device_id={fx_name: fx + 1 if which == RIGHT else fx - 1},
            device_id_type=MESH,
        )

    def arrival(c, which, slot):
        src, dst = sides[which]
        return pltpu.make_async_remote_copy(
            src_ref=src.at[c],
            dst_ref=dst.at[slot, c],
            send_sem=send_sem.at[2 + which],
            recv_sem=side_recv.at[which, slot, c],
            device_id={fx_name: fx + 1 if which == RIGHT else fx - 1},
            device_id_type=MESH,
        )

    def onward(c, which):
        _, dst = sides[which]
        return pltpu.make_async_remote_copy(
            src_ref=dst.at[PASSING, c],
            dst_ref=dst.at[HERE, c],
            send_sem=via_send.at[which, c],
            recv_sem=side_recv.at[which, HERE, c],
            device_id={fx_name: fx + 2 if which == RIGHT else fx - 2},
            device_id_type=MESH,
        )

    def stage_via(ways, k):
        for j in range(n):
            c = k * n + j

            @pl.when(passes_on(c, ways[0]))
            def _(c=c):
                for way in ways:
                    arrival(c, way, PASSING).wait_recv()
                    onward(c, way).start()

    load(0, 0).start()
    for i in range(4):
        constant(i).start()

    def loads(k, carry):
        load(k, 0).start()
        return carry

    def more_loads(k, carry):
        load(k, 1).start()
        load(k, 2).start()
        return carry

    def load_others():
        lax.fori_loop(1, chunks, loads, 0)
        for i in range(4, 9):
            constant(i).start()
        lax.fori_loop(0, chunks, more_loads, 0)

    acc[...] = jnp.zeros_like(acc)
    xs = lax.broadcasted_iota(jnp.int32, (tx, ty), 0)
    ys = lax.broadcasted_iota(jnp.int32, (tx, ty), 1)
    ax = jnp.where((xs >= tx - border) & has_right, 0.5**0.5, 1.0).astype(F32)
    by = jnp.where((ys >= ty - border) & has_down, 0.5**0.5, 1.0).astype(F32)
    weight[...] = ax * by

    peers = n_ch - 1
    for at, size in ((fy, n_fy), (fx, n_fx)):
        peers = peers + jnp.minimum(at, 1) + jnp.minimum(size - 1 - at, 1)
    peers = peers + jnp.minimum(fx // 2, 1) + jnp.minimum((n_fx - 1 - fx) // 2, 1)

    def own_edge(rows):
        at = lanes_of(rows)
        return (at >= tail - border) & (at < tail)

    half_lane = LANES // 2

    def members(k):
        return [k * n + j for j in range(n)]

    def stage_a(k, first=False):
        load(k, 0).wait()

        if first:
            for i in range(4):
                constant(i).wait()
            load_others()

        x = dual[part(k)]
        hx, hy = ex // 2, ey // 2
        corner = corner_step(x[:, :hx, :hy], sy1_ref[...], sx1_ref[...])
        full = jnp.stack(
            [
                jnp.concatenate(
                    [jnp.concatenate([corner[j], x[j, :hx, hy:]], axis=1), x[j, hx:]], axis=0
                )
                for j in range(n)
            ]
        )
        mid = times_right(full, sy0_ref[...])
        for j in range(n):
            work[k * n + j] = times_left(sx0_ref[...], mid[j])

        if first:
            pl.semaphore_wait(barrier, peers)

        @pl.when(has_up)
        def _():
            edge = own_edge(half)
            for c in members(k):
                first, second = work[c, :half, LANES:], work[c, half:, LANES:]
                y1s[c] = jnp.where(edge, roll(first, -border), roll(second, half_lane - border))
            for c in members(k):
                link(c, UP).start()

        @pl.when(has_left)
        def _():
            for c in members(k):
                las[c] = work[c, :border, :LANES]
            for c in members(k):
                to_side(c, LEFT_A).start()

    def stage_b(k):
        @pl.when(has_down)
        def _():
            for c in members(k):
                link(c, UP).wait_recv()
            edge = own_edge(half)
            for c in members(k):
                got = y1r[c]
                work[c, :half, LANES:] += jnp.where(edge, got, 0.0)
                work[c, half:, LANES:] += jnp.where(edge, roll(got, half_lane), 0.0)

        @pl.when(has_left)
        def _():
            for c in members(k):
                pack_rest(work[c, :border, LANES:], tail, lbs, c, 0)
            for c in members(k):
                to_side(c, LEFT_B).start()

    def stage_c(k):
        load(k, 1).wait()
        load(k, 2).wait()

        @pl.when(has_right)
        def _():
            for c in members(k):
                arrival(c, LEFT_A, HERE).wait_recv()
                arrival(c, LEFT_B, HERE).wait_recv()
            for c in members(k):
                work[c, ex - border:, :LANES] += lar[HERE, c]
                work[c, ex - border:, LANES:] += unpack_rest(lbr.at[HERE], c, 0, border, tail)

        for c in members(k):
            adjoint = work[c, border:, :ty] * weight[...]
            current = image[c]
            fresh = jnp.maximum(current - TAU_STEP * (grad[c].astype(F32) + adjoint), 0.0)
            work[c, border:, :ty] = (2.0 * fresh - current) * weight[...]
            next_ref[c] = fresh

        @pl.when(has_right)
        def _():
            for c in members(k):
                rs[c, :border] = work[c, ex - border:, :LANES]
                pack_rest(work[c, ex - border:, LANES:], tail, rs, c, border)
            for c in members(k):
                to_side(c, RIGHT).start()

        @pl.when(has_down)
        def _():
            mid = border + own_half
            edge = own_edge(own_half)
            for c in members(k):
                y2s[c, corner_half:] = jnp.where(
                    edge, work[c, border:mid, LANES:], roll(work[c, mid:, LANES:], half_lane)
                )
            for c in members(k):
                link(c, DOWN_A).start()

    def part_d(some):
        @pl.when(has_left)
        def _():
            for c in some:
                arrival(c, RIGHT, HERE).wait_recv()
            for c in some:
                work[c, :border, :LANES] = rr[HERE, c, :border]
                work[c, :border, LANES:] = unpack_rest(rr.at[HERE], c, border, border, tail)

        @pl.when(jnp.logical_not(has_left))
        def _():
            for c in some:
                work[c, :border] = jnp.zeros((border, ey), F32)

        @pl.when(has_down)
        def _():
            edge = own_edge(corner_half)
            for c in some:
                y2s[c, :corner_half] = jnp.where(
                    edge,
                    work[c, :corner_half, LANES:],
                    roll(work[c, corner_half:border, LANES:], half_lane),
                )
            for c in some:
                link(c, DOWN_B).start()

    def stage_d(k):
        for j in range(0, n, SUB):
            part_d(members(k)[j:j + SUB])

    def stage_e(k):
        @pl.when(k == 0)
        def _():
            for i in range(4, 8):
                constant(i).wait()

        @pl.when(has_up)
        def _():
            for c in members(k):
                link(c, DOWN_A).wait_recv()
                link(c, DOWN_B).wait_recv()
            for at, rows, buffered in ((0, corner_half, 0), (border, own_half, corner_half)):
                low = lanes_of(rows) < tail
                first, second = pl.ds(at, rows), pl.ds(at + rows, rows)
                for c in members(k):
                    got = y2r[c, buffered:buffered + rows]
                    work[c, first, LANES:] = jnp.where(low, work[c, first, LANES:], roll(got, border))
                    work[c, second, LANES:] = jnp.where(
                        low, work[c, second, LANES:], roll(got, border - half_lane)
                    )

        @pl.when(jnp.logical_not(has_up))
        def _():
            low = lanes_of(ex) < tail
            for c in members(k):
                work[c, :, LANES:] = jnp.where(low, work[c, :, LANES:], 0.0)

        mid = times_right(work[part(k)], ay0_ref[...])
        hx, hy = ex // 2, ey // 2
        full = [times_left(ax0_ref[...], mid[j]) for j in range(n)]
        corner = corner_step(jnp.stack([f[:hx, :hy] for f in full]), ay1_ref[...], ax1_ref[...])
        total = acc[...]
        for j in range(n):
            c = k * n + j
            coeffs = jnp.concatenate(
                [jnp.concatenate([corner[j], full[j][:hx, hy:]], axis=1), full[j][hx:]], axis=0
            )
            updated = dual[c] + coeffs
            total = total + updated * updated
            upd_ref[c] = updated
        acc[...] = total

    stages = (
        (0, stage_a),
        (1, stage_b),
        (2, functools.partial(stage_via, (LEFT_A, LEFT_B))),
        (3, stage_c),
        (4, functools.partial(stage_via, (RIGHT,))),
        (5, stage_d),
        (6, stage_e),
    )

    stage_a(0, True)

    def step(t, carry):
        for delay, stage in stages:
            early = 1 if stage is stage_a else 0

            @pl.when((t >= delay + early) & (t < chunks + delay))
            def _(delay=delay, stage=stage):
                stage(t - delay)
        return carry

    lax.fori_loop(0, chunks + 6, step, 0)

    def across(step):
        return pltpu.make_async_remote_copy(
            src_ref=acc,
            dst_ref=accr.at[step - 1],
            send_sem=ch_send.at[step - 1],
            recv_sem=ch_recv.at[step - 1],
            device_id={ch_name: lax.rem(ch + step, n_ch)},
            device_id_type=MESH,
        )

    for s in range(1, n_ch):
        across(s).start()
    for which, there in ((UP, has_up), (DOWN_A, has_down)):
        @pl.when(there)
        def _(which=which):
            link_sent(which).wait_send()
    for which, there in ((LEFT_A, has_left), (LEFT_B, has_left), (RIGHT, has_right)):
        @pl.when(there)
        def _(which=which):
            side_sent(which).wait_send()

    def passed(c, carry):
        for ways in ((LEFT_A, LEFT_B), (RIGHT,)):
            @pl.when(passes_on(c, ways[0]))
            def _(ways=ways):
                for way in ways:
                    onward(c, way).wait_send()
        return carry

    lax.fori_loop(0, channels, passed, 0)
    constant(8).wait()
    for s in range(1, n_ch):
        across(s).wait()
    total = acc[...]
    for s in range(1, n_ch):
        total = total + accr[s - 1]
    factor_ref[...] = jnp.minimum(1.0, LAMBDA_REG * rew_ref[...] / jnp.sqrt(total + EPSILON))


def finish(image_ref, upd_ref, factor_ref, next_hbm, dual_hbm, scaled, sem):
    channels = upd_ref.shape[0]
    n = channels // PIECES

    def image_out(i):
        at = pl.ds(i * n, n)
        return pltpu.make_async_copy(image_ref.at[at], next_hbm.at[at], sem.at[0, i])

    def dual_out(i):
        at = pl.ds(i * n, n)
        return pltpu.make_async_copy(scaled.at[at], dual_hbm.at[at], sem.at[1, i])

    for i in range(PIECES):
        image_out(i).start()

    def piece(i, carry):
        for j in range(n):
            scaled[i * n + j] = upd_ref[i * n + j] * factor_ref[...]
        dual_out(i).start()
        return carry

    lax.fori_loop(0, PIECES, piece, 0)
    for i in range(PIECES):
        image_out(i).wait()
        dual_out(i).wait()


def shards(names, image_cube, data_grad, dual_coeffs, reweights):
    channels, tx, ty = image_cube.shape
    _, ex, ey = dual_coeffs.shape
    border = ex - tx
    n_ch = lax.axis_size(names[2])
    chunks = channels // CHUNK
    rest = packed_rows(border, ty - LANES)
    wy0 = np.roll(level_matrix(ey), -(ey - ty), axis=1)
    wx0 = level_matrix(ex)
    wy1, wx1 = level_matrix(ey // 2), level_matrix(ex // 2)
    px0, px1 = round_up(ex, 16), round_up(ex // 2, 16)
    factors = (
        right_factor(wy0), left_factor(wx0.T, px0), right_factor(wy1), left_factor(wx1.T, px1),
        right_factor(wy0.T), left_factor(wx0, px0), right_factor(wy1.T), left_factor(wx1, px1),
    )
    far = pl.BlockSpec(memory_space=pltpu.HBM)
    inside = pl.BlockSpec(memory_space=pltpu.VMEM)
    lines = pltpu.VMEM((channels, ex // 2, LANES), F32)
    side_rows = (border, rest, border + rest)
    side_bufs = [
        pltpu.VMEM(shape, F32)
        for rows in side_rows
        for shape in ((channels, rows, LANES), (2, channels, rows, LANES))
    ]
    operands = (image_cube, data_grad, dual_coeffs, reweights, *factors)
    image_next, updated, factor = pl.pallas_call(
        functools.partial(kernel, names),
        out_shape=(
            pltpu.VMEM((channels, tx, ty), F32),
            pltpu.VMEM((channels, ex, ey), F32),
            pltpu.VMEM((ex, ey), F32),
        ),
        in_specs=[far] * len(operands),
        out_specs=(inside,) * 3,
        scratch_shapes=[
            *(pltpu.VMEM(f.shape, f.dtype) for f in factors),
            pltpu.VMEM((ex, ey), F32),
            pltpu.VMEM((channels, tx, ty), F32),
            pltpu.VMEM((channels, tx, ty), BF16),
            pltpu.VMEM((channels, ex, ey), F32),
            pltpu.VMEM((channels, ex, ey), F32),
            pltpu.VMEM((tx, ty), F32),
            lines, lines, *side_bufs, lines, lines,
            pltpu.VMEM((ex, ey), F32),
            pltpu.VMEM((n_ch - 1, ex, ey), F32),
            pltpu.SemaphoreType.DMA((3, chunks)),
            pltpu.SemaphoreType.DMA((9,)),
            pltpu.SemaphoreType.DMA((5,)),
            pltpu.SemaphoreType.DMA((3, channels)),
            pltpu.SemaphoreType.DMA((3, 2, channels)),
            pltpu.SemaphoreType.DMA((3, channels)),
            pltpu.SemaphoreType.DMA((n_ch - 1,)),
            pltpu.SemaphoreType.DMA((n_ch - 1,)),
        ],
        compiler_params=pltpu.CompilerParams(
            collective_id=0, has_side_effects=True, vmem_limit_bytes=40 * 2**20
        ),
        name="facets",
    )(*(pltpu.with_memory_space_constraint(a, pltpu.HBM) for a in operands))
    anywhere = pl.BlockSpec(memory_space=pl.ANY)
    return pl.pallas_call(
        finish,
        out_shape=(
            jax.ShapeDtypeStruct((channels, tx, ty), F32),
            jax.ShapeDtypeStruct((channels, ex, ey), F32),
        ),
        in_specs=[inside] * 3,
        out_specs=(anywhere, anywhere),
        scratch_shapes=[
            pltpu.VMEM((channels, ex, ey), F32),
            pltpu.SemaphoreType.DMA((2, PIECES)),
        ],
        compiler_params=pltpu.CompilerParams(vmem_limit_bytes=40 * 2**20),
        name="finish",
    )(*(pltpu.with_memory_space_constraint(a, pltpu.VMEM) for a in (image_next, updated, factor)))


def solution(mesh):
    names = ("fy", "fx", "ch")
    return jax.shard_map(
        functools.partial(shards, names),
        mesh=mesh,
        in_specs=(P("ch", "fx", "fy"), P("ch", "fx", "fy"), P("ch", "fx", "fy"), P("fx", "fy")),
        out_specs=(P("ch", "fx", "fy"), P("ch", "fx", "fy")),
        check_vma=False,
    )
```

```python
import functools

import jax
import jax.numpy as jnp
import numpy as np
from jax import lax
from jax.experimental import pallas as pl
from jax.experimental.pallas import tpu as pltpu
from jax.sharding import PartitionSpec as P

LEVELS = 2
LOW_PASS = [
    -0.00011747678400228192,
    0.0006754494059985568,
    -0.0003917403729959771,
    -0.00487035299301066,
    0.008746094047015655,
    0.013981027917015516,
    -0.04408825393106472,
    -0.01736930100202211,
    0.128747426620186,
    0.00047248457399797254,
    -0.2840155429624281,
    -0.015829105256023893,
    0.5853546836548691,
    0.6756307362980128,
    0.3128715909144659,
    0.05441584224308161,
]
TAU_STEP = 0.5
LAMBDA_REG = 1.0
EPSILON = 1e-06
LANES = 128
SUBLANES = 8
PIECES = 8
SUB = 2
CHUNK = 4
AT_B, AT_VIA_L, AT_C, AT_VIA_R, AT_D, AT_E = 2, 3, 4, 7, 8, 9
MESH = pl.DeviceIdType.MESH
F32 = jnp.float32
BF16 = jnp.bfloat16


def level_matrix(length):
    halved = length // 2
    taps_count = len(LOW_PASS)
    matrix = np.zeros((length, length))
    for out_row in range(halved):
        for tap_index in range(taps_count):
            column = (2 * out_row + tap_index) % length
            matrix[out_row, column] += LOW_PASS[tap_index]
            matrix[halved + out_row, column] += (-1) ** tap_index * LOW_PASS[
                taps_count - 1 - tap_index
            ]
    return matrix


def halves(matrix):
    exact = np.asarray(matrix, np.float32)
    high = exact.astype(BF16)
    low = (exact - high.astype(np.float32)).astype(BF16)
    return high, low


def right_factor(matrix):
    high, low = halves(matrix)
    return jnp.asarray(np.concatenate([high, low, high], axis=0))


def left_factor(matrix, padded):
    high, low = halves(np.pad(matrix, ((0, 0), (0, padded - matrix.shape[1]))))
    return jnp.asarray(np.concatenate([high, low, high], axis=1))


def round_up(value, to):
    return -(-value // to) * to


def split(x):
    high = x.astype(BF16)
    low = (x - high.astype(F32)).astype(BF16)
    return high, low


def times_right(x, factor):
    n, rows, columns = x.shape
    high, low = split(x.reshape(n * rows, columns))
    out = jnp.dot(jnp.concatenate([high, high, low], axis=1), factor, preferred_element_type=F32)
    return out.reshape(n, rows, out.shape[1])


def times_left(factor, x):
    rows = x.shape[0]
    padded = round_up(rows, 16)
    if padded > rows:
        x = jnp.concatenate([x, jnp.zeros((padded - rows, x.shape[1]), F32)], axis=0)
    high, low = split(x)
    return jnp.dot(factor, jnp.concatenate([high, high, low], axis=0), preferred_element_type=F32)


def corner_step(corner, right, left):
    n = corner.shape[0]
    width = corner.shape[2]
    mid = times_right(corner, right)
    pieces = []
    for c in range(0, n, 2):
        pair = times_left(left, jnp.concatenate([mid[c], mid[c + 1]], axis=1))
        pieces += [pair[:, :width], pair[:, width:]]
    return pieces


def lanes_of(rows):
    return lax.broadcasted_iota(jnp.int32, (rows, LANES), 1)


def roll(x, by):
    return pltpu.roll(x, by % LANES, 1)


def seats(border, tail):
    groups = border // SUBLANES
    bins = -(-groups * tail // LANES)
    last = groups * tail - (bins - 1) * LANES
    pieces, seat, at = [], 0, tail
    for group in range(bins, groups):
        lane = 0
        while lane < tail:
            room = LANES if seat < bins - 1 else last
            if at == room:
                seat, at = seat + 1, tail
                continue
            width = min(tail - lane, room - at)
            pieces.append((group, lane, seat, at))
            lane, at = lane + width, at + width
    spare = LANES - last
    kept = SUBLANES * last // LANES
    folds = []
    if spare:
        assert last % spare == 0 and (SUBLANES - kept) * last == spare * kept
        folds = [(row, (row - kept) * (last // spare)) for row in range(kept, SUBLANES)]
    return groups, bins, last, kept, pieces, folds


def packed_rows(border, tail):
    _, bins, _, kept, _, _ = seats(border, tail)
    return (bins - 1) * SUBLANES + kept


def pack_rest(rest, tail, buffer, c, start):
    groups, bins, last, kept, pieces, folds = seats(rest.shape[0], tail)
    lane = lanes_of(SUBLANES)
    row = lax.broadcasted_iota(jnp.int32, (SUBLANES, LANES), 0)
    part = [rest[SUBLANES * i:SUBLANES * (i + 1)] for i in range(groups)]
    out = part[:bins]
    for group, source, seat, to in pieces:
        out[seat] = jnp.where(lane >= to, roll(part[group], to - source), out[seat])
    spare = LANES - last
    end = out[-1]
    for step in range(last // spare if folds else 0):
        moved = roll(out[-1], last - spare * step)
        for i, first in folds:
            line = jnp.broadcast_to(moved[i:i + 1], (SUBLANES, LANES))
            end = jnp.where((lane >= last) & (row == first + step), line, end)
    for i in range(bins - 1):
        buffer[c, start + SUBLANES * i:start + SUBLANES * (i + 1)] = out[i]
    start += SUBLANES * (bins - 1)
    buffer[c, start:start + kept] = end[:kept]


def unpack_rest(buffer, c, start, border, tail):
    groups, bins, last, kept, pieces, folds = seats(border, tail)
    lane = lanes_of(SUBLANES)
    row = lax.broadcasted_iota(jnp.int32, (SUBLANES, LANES), 0)
    part = [buffer[c, start + SUBLANES * i:start + SUBLANES * (i + 1)] for i in range(bins - 1)]
    start += SUBLANES * (bins - 1)
    end = buffer[c, start:start + kept]
    if folds:
        end = jnp.concatenate([end, end[:SUBLANES - kept]], axis=0)
    spare = LANES - last
    whole = end
    for step in range(last // spare if folds else 0):
        moved = roll(end, spare * step - last)
        for i, first in folds:
            line = jnp.broadcast_to(moved[first + step:first + step + 1], (SUBLANES, LANES))
            whole = jnp.where((lane >= step * spare) & (row == i), line, whole)
    part.append(whole)
    for group in range(bins, groups):
        found = None
        for owner, source, seat, to in pieces:
            if owner == group:
                moved = roll(part[seat], source - to)
                found = moved if found is None else jnp.where(lane >= source, moved, found)
        part.append(found)
    return jnp.concatenate(part, axis=0)


def kernel(
    names,
    image_hbm, grad_hbm, dual_hbm, rew_hbm,
    sy0_hbm, sx0_hbm, sy1_hbm, sx1_hbm, ay0_hbm, ax0_hbm, ay1_hbm, ax1_hbm,
    next_ref, upd_ref, factor_ref,
    sy0_ref, sx0_ref, sy1_ref, sx1_ref, ay0_ref, ax0_ref, ay1_ref, ax1_ref, rew_ref,
    image, grad, dual, work, weight, y1s, y1r, las, lar, lbs, lbr, rs, rr, y2s, y2r, acc, accr,
    in_sem, const_sem, send_sem, recv_sem, side_recv, via_send, ch_send, ch_recv,
):
    fy_name, fx_name, ch_name = names
    channels, tx, ty = image.shape
    ex, ey = dual.shape[1:]
    border = ex - tx
    n = CHUNK
    chunks = channels // n
    half = ex // 2
    tail = ty - LANES
    fy, fx, ch = (lax.axis_index(a) for a in names)
    n_fy, n_fx, n_ch = (lax.axis_size(a) for a in names)
    has_up, has_down = fy > 0, fy < n_fy - 1
    has_left, has_right = fx > 0, fx < n_fx - 1

    barrier = pltpu.get_barrier_semaphore()
    near = (
        (has_up, {fy_name: fy - 1}),
        (has_down, {fy_name: fy + 1}),
        (has_left, {fx_name: fx - 1}),
        (has_right, {fx_name: fx + 1}),
        (fx > 1, {fx_name: fx - 2}),
        (fx < n_fx - 2, {fx_name: fx + 2}),
    )
    for there, where in near:
        @pl.when(there)
        def _(where=where):
            pl.semaphore_signal(barrier, inc=1, device_id=where, device_id_type=MESH)
    for step in range(1, n_ch):
        pl.semaphore_signal(
            barrier, inc=1, device_id={ch_name: lax.rem(ch + step, n_ch)}, device_id_type=MESH
        )

    def part(k):
        return pl.ds(k * n, n)

    def load(k, which):
        src, dst = ((dual_hbm, dual), (image_hbm, image), (grad_hbm, grad))[which]
        return pltpu.make_async_copy(src.at[part(k)], dst.at[part(k)], in_sem.at[which, k])

    constants = (
        (sy1_hbm, sy1_ref), (sx1_hbm, sx1_ref), (sy0_hbm, sy0_ref), (sx0_hbm, sx0_ref),
        (ay0_hbm, ay0_ref), (ax0_hbm, ax0_ref), (ay1_hbm, ay1_ref), (ax1_hbm, ax1_ref),
        (rew_hbm, rew_ref),
    )

    def constant(i):
        src, dst = constants[i]
        return pltpu.make_async_copy(src, dst, const_sem.at[i])

    corner_half, own_half = border // 2, tx // 2
    corner_rows, own_rows = pl.ds(0, corner_half), pl.ds(corner_half, own_half)
    links = (
        (y1s, y1r, {fy_name: fy - 1}, None),
        (y2s, y2r, {fy_name: fy + 1}, own_rows),
        (y2s, y2r, {fy_name: fy + 1}, corner_rows),
    )
    UP, DOWN_A, DOWN_B = range(3)
    sides = ((las, lar), (lbs, lbr), (rs, rr))
    LEFT_A, LEFT_B, RIGHT = range(3)
    HERE, PASSING = 0, 1

    def link(c, which):
        src, dst, where, rows = links[which]
        return pltpu.make_async_remote_copy(
            src_ref=src.at[c] if rows is None else src.at[c, rows],
            dst_ref=dst.at[c] if rows is None else dst.at[c, rows],
            send_sem=send_sem.at[min(which, 1)],
            recv_sem=recv_sem.at[which, c],
            device_id=where,
            device_id_type=MESH,
        )

    def link_sent(which):
        src, dst, where, _ = links[which]
        return pltpu.make_async_remote_copy(
            src_ref=src,
            dst_ref=dst,
            send_sem=send_sem.at[min(which, 1)],
            recv_sem=recv_sem.at[which, 0],
            device_id=where,
            device_id_type=MESH,
        )

    odd = lax.rem(fx, 2) == 1
    groups = n_fx // 2

    def sends_via(c, which):
        if which != RIGHT:
            return jnp.logical_not(odd) & has_left & has_right & (lax.rem(c, groups) >= groups - fx // 2)
        return odd & has_left & has_right & (lax.rem(c, groups) >= (fx + 1) // 2)

    def passes_on(c, which):
        if which != RIGHT:
            return odd & (fx > 2) & (lax.rem(c, groups) >= groups - fx // 2)
        return jnp.logical_not(odd) & (fx < n_fx - 2) & (lax.rem(c, groups) >= (fx + 2) // 2)

    def to_side(c, which):
        src, dst = sides[which]
        ahead, back = (fx + 1, fx - 1) if which == RIGHT else (fx - 1, fx + 1)
        around = sends_via(c, which)
        slot = jnp.where(around, PASSING, HERE)
        return pltpu.make_async_remote_copy(
            src_ref=src.at[c],
            dst_ref=dst.at[slot, c],
            send_sem=send_sem.at[2 + which],
            recv_sem=side_recv.at[which, slot, c],
            device_id={fx_name: jnp.where(around, back, ahead)},
            device_id_type=MESH,
        )

    def side_sent(which):
        src, dst = sides[which]
        return pltpu.make_async_remote_copy(
            src_ref=src,
            dst_ref=dst.at[HERE],
            send_sem=send_sem.at[2 + which],
            recv_sem=side_recv.at[which, HERE, 0],
            device_id={fx_name: fx + 1 if which == RIGHT else fx - 1},
            device_id_type=MESH,
        )

    def arrival(c, which, slot):
        src, dst = sides[which]
        return pltpu.make_async_remote_copy(
            src_ref=src.at[c],
            dst_ref=dst.at[slot, c],
            send_sem=send_sem.at[2 + which],
            recv_sem=side_recv.at[which, slot, c],
            device_id={fx_name: fx + 1 if which == RIGHT else fx - 1},
            device_id_type=MESH,
        )

    def onward(c, which):
        _, dst = sides[which]
        return pltpu.make_async_remote_copy(
            src_ref=dst.at[PASSING, c],
            dst_ref=dst.at[HERE, c],
            send_sem=via_send.at[which, c],
            recv_sem=side_recv.at[which, HERE, c],
            device_id={fx_name: fx + 2 if which == RIGHT else fx - 2},
            device_id_type=MESH,
        )

    def stage_via(ways, k):
        for j in range(n):
            c = k * n + j

            @pl.when(passes_on(c, ways[0]))
            def _(c=c):
                for way in ways:
                    arrival(c, way, PASSING).wait_recv()
                    onward(c, way).start()

    load(0, 0).start()
    for i in range(4):
        constant(i).start()

    def loads(k, carry):
        load(k, 0).start()
        return carry

    def more_loads(k, carry):
        load(k, 1).start()
        load(k, 2).start()
        return carry

    def load_others():
        lax.fori_loop(1, chunks, loads, 0)
        for i in range(4, 9):
            constant(i).start()
        lax.fori_loop(0, chunks, more_loads, 0)

    acc[...] = jnp.zeros_like(acc)
    xs = lax.broadcasted_iota(jnp.int32, (tx, ty), 0)
    ys = lax.broadcasted_iota(jnp.int32, (tx, ty), 1)
    ax = jnp.where((xs >= tx - border) & has_right, 0.5**0.5, 1.0).astype(F32)
    by = jnp.where((ys >= ty - border) & has_down, 0.5**0.5, 1.0).astype(F32)
    weight[...] = ax * by

    peers = n_ch - 1
    for at, size in ((fy, n_fy), (fx, n_fx)):
        peers = peers + jnp.minimum(at, 1) + jnp.minimum(size - 1 - at, 1)
    peers = peers + jnp.minimum(fx // 2, 1) + jnp.minimum((n_fx - 1 - fx) // 2, 1)

    def own_edge(rows):
        at = lanes_of(rows)
        return (at >= tail - border) & (at < tail)

    half_lane = LANES // 2

    def members(k):
        return [k * n + j for j in range(n)]

    def stage_a(k, first=False):
        load(k, 0).wait()

        if first:
            for i in range(4):
                constant(i).wait()
            load_others()

        x = dual[part(k)]
        hx, hy = ex // 2, ey // 2
        corner = corner_step(x[:, :hx, :hy], sy1_ref[...], sx1_ref[...])
        full = jnp.stack(
            [
                jnp.concatenate(
                    [jnp.concatenate([corner[j], x[j, :hx, hy:]], axis=1), x[j, hx:]], axis=0
                )
                for j in range(n)
            ]
        )
        mid = times_right(full, sy0_ref[...])
        for j in range(n):
            work[k * n + j] = times_left(sx0_ref[...], mid[j])

        if first:
            pl.semaphore_wait(barrier, peers)

        @pl.when(has_up)
        def _():
            edge = own_edge(half)
            for c in members(k):
                first, second = work[c, :half, LANES:], work[c, half:, LANES:]
                y1s[c] = jnp.where(edge, roll(first, -border), roll(second, half_lane - border))
            for c in members(k):
                link(c, UP).start()

        @pl.when(has_left)
        def _():
            for c in members(k):
                las[c] = work[c, :border, :LANES]
            for c in members(k):
                to_side(c, LEFT_A).start()

    def stage_b(k):
        @pl.when(has_down)
        def _():
            for c in members(k):
                link(c, UP).wait_recv()
            edge = own_edge(half)
            for c in members(k):
                got = y1r[c]
                work[c, :half, LANES:] += jnp.where(edge, got, 0.0)
                work[c, half:, LANES:] += jnp.where(edge, roll(got, half_lane), 0.0)

        @pl.when(has_left)
        def _():
            for c in members(k):
                pack_rest(work[c, :border, LANES:], tail, lbs, c, 0)
            for c in members(k):
                to_side(c, LEFT_B).start()

    def stage_c(k):
        load(k, 1).wait()
        load(k, 2).wait()

        @pl.when(has_right)
        def _():
            for c in members(k):
                arrival(c, LEFT_A, HERE).wait_recv()
                arrival(c, LEFT_B, HERE).wait_recv()
            for c in members(k):
                work[c, ex - border:, :LANES] += lar[HERE, c]
                work[c, ex - border:, LANES:] += unpack_rest(lbr.at[HERE], c, 0, border, tail)

        for c in members(k):
            adjoint = work[c, border:, :ty] * weight[...]
            current = image[c]
            fresh = jnp.maximum(current - TAU_STEP * (grad[c].astype(F32) + adjoint), 0.0)
            work[c, border:, :ty] = (2.0 * fresh - current) * weight[...]
            next_ref[c] = fresh

        @pl.when(has_right)
        def _():
            for c in members(k):
                rs[c, :border] = work[c, ex - border:, :LANES]
                pack_rest(work[c, ex - border:, LANES:], tail, rs, c, border)
            for c in members(k):
                to_side(c, RIGHT).start()

        @pl.when(has_down)
        def _():
            mid = border + own_half
            edge = own_edge(own_half)
            for c in members(k):
                y2s[c, corner_half:] = jnp.where(
                    edge, work[c, border:mid, LANES:], roll(work[c, mid:, LANES:], half_lane)
                )
            for c in members(k):
                link(c, DOWN_A).start()

    def part_d(some):
        @pl.when(has_left)
        def _():
            for c in some:
                arrival(c, RIGHT, HERE).wait_recv()
            for c in some:
                work[c, :border, :LANES] = rr[HERE, c, :border]
                work[c, :border, LANES:] = unpack_rest(rr.at[HERE], c, border, border, tail)

        @pl.when(jnp.logical_not(has_left))
        def _():
            for c in some:
                work[c, :border] = jnp.zeros((border, ey), F32)

        @pl.when(has_down)
        def _():
            edge = own_edge(corner_half)
            for c in some:
                y2s[c, :corner_half] = jnp.where(
                    edge,
                    work[c, :corner_half, LANES:],
                    roll(work[c, corner_half:border, LANES:], half_lane),
                )
            for c in some:
                link(c, DOWN_B).start()

    def stage_d(k):
        for j in range(0, n, SUB):
            part_d(members(k)[j:j + SUB])

    def stage_e(k):
        @pl.when(k == 0)
        def _():
            for i in range(4, 8):
                constant(i).wait()

        @pl.when(has_up)
        def _():
            for c in members(k):
                link(c, DOWN_A).wait_recv()
                link(c, DOWN_B).wait_recv()
            for at, rows, buffered in ((0, corner_half, 0), (border, own_half, corner_half)):
                low = lanes_of(rows) < tail
                first, second = pl.ds(at, rows), pl.ds(at + rows, rows)
                for c in members(k):
                    got = y2r[c, buffered:buffered + rows]
                    work[c, first, LANES:] = jnp.where(low, work[c, first, LANES:], roll(got, border))
                    work[c, second, LANES:] = jnp.where(
                        low, work[c, second, LANES:], roll(got, border - half_lane)
                    )

        @pl.when(jnp.logical_not(has_up))
        def _():
            low = lanes_of(ex) < tail
            for c in members(k):
                work[c, :, LANES:] = jnp.where(low, work[c, :, LANES:], 0.0)

        mid = times_right(work[part(k)], ay0_ref[...])
        hx, hy = ex // 2, ey // 2
        full = [times_left(ax0_ref[...], mid[j]) for j in range(n)]
        corner = corner_step(jnp.stack([f[:hx, :hy] for f in full]), ay1_ref[...], ax1_ref[...])
        total = acc[...]
        for j in range(n):
            c = k * n + j
            coeffs = jnp.concatenate(
                [jnp.concatenate([corner[j], full[j][:hx, hy:]], axis=1), full[j][hx:]], axis=0
            )
            updated = dual[c] + coeffs
            total = total + updated * updated
            upd_ref[c] = updated
        acc[...] = total

    stages = (
        (0, stage_a),
        (1, stage_b),
        (2, functools.partial(stage_via, (LEFT_A, LEFT_B))),
        (3, stage_c),
        (4, functools.partial(stage_via, (RIGHT,))),
        (5, stage_d),
        (6, stage_e),
    )

    stage_a(0, True)

    def step(t, carry):
        for delay, stage in stages:
            early = 1 if stage is stage_a else 0

            @pl.when((t >= delay + early) & (t < chunks + delay))
            def _(delay=delay, stage=stage):
                stage(t - delay)
        return carry

    lax.fori_loop(0, chunks + 6, step, 0)

    def across(step):
        return pltpu.make_async_remote_copy(
            src_ref=acc,
            dst_ref=accr.at[step - 1],
            send_sem=ch_send.at[step - 1],
            recv_sem=ch_recv.at[step - 1],
            device_id={ch_name: lax.rem(ch + step, n_ch)},
            device_id_type=MESH,
        )

    for s in range(1, n_ch):
        across(s).start()
    for which, there in ((UP, has_up), (DOWN_A, has_down)):
        @pl.when(there)
        def _(which=which):
            link_sent(which).wait_send()
    for which, there in ((LEFT_A, has_left), (LEFT_B, has_left), (RIGHT, has_right)):
        @pl.when(there)
        def _(which=which):
            side_sent(which).wait_send()

    def passed(c, carry):
        for ways in ((LEFT_A, LEFT_B), (RIGHT,)):
            @pl.when(passes_on(c, ways[0]))
            def _(ways=ways):
                for way in ways:
                    onward(c, way).wait_send()
        return carry

    lax.fori_loop(0, channels, passed, 0)
    constant(8).wait()
    for s in range(1, n_ch):
        across(s).wait()
    total = acc[...]
    for s in range(1, n_ch):
        total = total + accr[s - 1]
    factor_ref[...] = jnp.minimum(1.0, LAMBDA_REG * rew_ref[...] / jnp.sqrt(total + EPSILON))


def finish(image_ref, upd_ref, factor_ref, next_hbm, dual_hbm, scaled, sem):
    channels = upd_ref.shape[0]
    n = channels // PIECES

    def image_out(i):
        at = pl.ds(i * n, n)
        return pltpu.make_async_copy(image_ref.at[at], next_hbm.at[at], sem.at[0, i])

    def dual_out(i):
        at = pl.ds(i * n, n)
        return pltpu.make_async_copy(scaled.at[at], dual_hbm.at[at], sem.at[1, i])

    for i in range(PIECES):
        image_out(i).start()

    def piece(i, carry):
        for j in range(n):
            scaled[i * n + j] = upd_ref[i * n + j] * factor_ref[...]
        dual_out(i).start()
        return carry

    lax.fori_loop(0, PIECES, piece, 0)
    for i in range(PIECES):
        image_out(i).wait()
        dual_out(i).wait()


def shards(names, image_cube, data_grad, dual_coeffs, reweights):
    channels, tx, ty = image_cube.shape
    _, ex, ey = dual_coeffs.shape
    border = ex - tx
    n_ch = lax.axis_size(names[2])
    chunks = channels // CHUNK
    rest = packed_rows(border, ty - LANES)
    wy0 = np.roll(level_matrix(ey), -(ey - ty), axis=1)
    wx0 = level_matrix(ex)
    wy1, wx1 = level_matrix(ey // 2), level_matrix(ex // 2)
    px0, px1 = round_up(ex, 16), round_up(ex // 2, 16)
    factors = (
        right_factor(wy0), left_factor(wx0.T, px0), right_factor(wy1), left_factor(wx1.T, px1),
        right_factor(wy0.T), left_factor(wx0, px0), right_factor(wy1.T), left_factor(wx1, px1),
    )
    far = pl.BlockSpec(memory_space=pltpu.HBM)
    inside = pl.BlockSpec(memory_space=pltpu.VMEM)
    lines = pltpu.VMEM((channels, ex // 2, LANES), F32)
    side_rows = (border, rest, border + rest)
    side_bufs = [
        pltpu.VMEM(shape, F32)
        for rows in side_rows
        for shape in ((channels, rows, LANES), (2, channels, rows, LANES))
    ]
    operands = (image_cube, data_grad, dual_coeffs, reweights, *factors)
    image_next, updated, factor = pl.pallas_call(
        functools.partial(kernel, names),
        out_shape=(
            pltpu.VMEM((channels, tx, ty), F32),
            pltpu.VMEM((channels, ex, ey), F32),
            pltpu.VMEM((ex, ey), F32),
        ),
        in_specs=[far] * len(operands),
        out_specs=(inside,) * 3,
        scratch_shapes=[
            *(pltpu.VMEM(f.shape, f.dtype) for f in factors),
            pltpu.VMEM((ex, ey), F32),
            pltpu.VMEM((channels, tx, ty), F32),
            pltpu.VMEM((channels, tx, ty), BF16),
            pltpu.VMEM((channels, ex, ey), F32),
            pltpu.VMEM((channels, ex, ey), F32),
            pltpu.VMEM((tx, ty), F32),
            lines, lines, *side_bufs, lines, lines,
            pltpu.VMEM((ex, ey), F32),
            pltpu.VMEM((n_ch - 1, ex, ey), F32),
            pltpu.SemaphoreType.DMA((3, chunks)),
            pltpu.SemaphoreType.DMA((9,)),
            pltpu.SemaphoreType.DMA((5,)),
            pltpu.SemaphoreType.DMA((3, channels)),
            pltpu.SemaphoreType.DMA((3, 2, channels)),
            pltpu.SemaphoreType.DMA((3, channels)),
            pltpu.SemaphoreType.DMA((n_ch - 1,)),
            pltpu.SemaphoreType.DMA((n_ch - 1,)),
        ],
        compiler_params=pltpu.CompilerParams(
            collective_id=0, has_side_effects=True, vmem_limit_bytes=40 * 2**20
        ),
        name="facets",
    )(*(pltpu.with_memory_space_constraint(a, pltpu.HBM) for a in operands))
    anywhere = pl.BlockSpec(memory_space=pl.ANY)
    return pl.pallas_call(
        finish,
        out_shape=(
            jax.ShapeDtypeStruct((channels, tx, ty), F32),
            jax.ShapeDtypeStruct((channels, ex, ey), F32),
        ),
        in_specs=[inside] * 3,
        out_specs=(anywhere, anywhere),
        scratch_shapes=[
            pltpu.VMEM((channels, ex, ey), F32),
            pltpu.SemaphoreType.DMA((2, PIECES)),
        ],
        compiler_params=pltpu.CompilerParams(vmem_limit_bytes=40 * 2**20),
        name="finish",
    )(*(pltpu.with_memory_space_constraint(a, pltpu.VMEM) for a in (image_next, updated, factor)))


def solution(mesh):
    names = ("fy", "fx", "ch")
    return jax.shard_map(
        functools.partial(shards, names),
        mesh=mesh,
        in_specs=(P("ch", "fx", "fy"), P("ch", "fx", "fy"), P("ch", "fx", "fy"), P("fx", "fy")),
        out_specs=(P("ch", "fx", "fy"), P("ch", "fx", "fy")),
        check_vma=False,
    )
```
